32 devices in a mesh: dp: 4 (over z), tensor: 8 (over y, x, core).
Axes of the slice: x: 2, y: 2, z: 4, core: 2. Of those that a mesh axis runs over, the one named last changes fastest.
Arguments:
- activations: bfloat16 [1024, 27648], P('dp', 'tensor'), may hold values from -6 to 6
- left_factor: float32 [216, 216], replicated, may hold values from -2 to 3, as said below
- right_factor: float32 [128, 128], replicated, may hold values from -2 to 3, as said below
- clip_scale: float32 [128, 216], replicated, may hold values from 0.5 to 3
- weight_rows: bfloat16 [27648, 5120], P('tensor'), may hold values from -0.0390625 to 0.0390625
- target: bfloat16 [1024, 5120], P('dp'), may hold values from -6 to 6
Outputs:
- grad_left: float32 [216, 216], replicated
- grad_right: float32 [128, 128], replicated
- grad_input: float32 [1024, 27648], P('dp', 'tensor')
The draws below stay inside these ranges and needn't reach their ends.
Inputs may be any that keep to these rules, and one draw needn't show every extreme that they name: `left_factor`: the identity plus independent entries of order one over the square root of 216. `right_factor`: the identity plus independent entries of order one over the square root of 128.
All inputs are finite; a program needn't handle non-finite values.
Results may differ from the reference program's by a relative error of at most 0.007.
Values may be sent and summed in bfloat16 or wider, within the bound.
A program may use at most 128 MiB of HBM per device.

```python
import math
import jax
import jax.numpy as jnp
from jax import lax

OUT = 5120
F1 = 216
F2 = 128
HID = 27648
TOKENS = 1024


def make_factor(key, order):
    noise = jnp.clip(jax.random.normal(key, (order, order), jnp.float32), -4.0, 4.0)
    return jnp.eye(order, dtype=jnp.float32) + noise / jnp.sqrt(order * 1.0)


def draw_left_factor(key, part):
    return make_factor(jax.random.fold_in(key, 11), F1)


def draw_right_factor(key, part):
    return make_factor(jax.random.fold_in(key, 23), F2)


def block_levels(key, shape, pieces, low, high):
    def one(dim, blocks):
        steps = jax.random.uniform(jax.random.fold_in(jax.random.fold_in(key, 6), dim), (blocks,), jnp.float32, low / len(pieces), high / len(pieces))
        return jnp.repeat(jnp.exp(steps), shape[dim] // blocks).reshape((-1,) + (1,) * (len(shape) - dim - 1))

    factor_of = one(*pieces[0])
    for cut in pieces[1:]:
        factor_of = factor_of * one(*cut)
    return factor_of


def normal_values(stream_key, shape, spread, bound, pieces=(), kind=jnp.bfloat16):
    loudness = block_levels(stream_key, shape, pieces, -0.22, 0.18) if pieces else 1.0
    values = jax.random.normal(stream_key, shape, jnp.float32) * spread * loudness
    return jnp.minimum(jnp.maximum(values, -bound), bound).astype(kind)


def setup_inputs(seed: int = 0) -> dict:
    seeds = jax.random.split(jax.random.key(seed), 7)
    activations = normal_values(seeds[0], (TOKENS, HID), 1.0, 6.0, ((0, 4), (1, 8)))
    left_factor = draw_left_factor(jax.random.fold_in(seeds[6], 71), 0)
    right_factor = draw_right_factor(jax.random.fold_in(seeds[6], 71), 0)
    clip_scale = jnp.clip(jnp.exp(jax.random.uniform(seeds[3], (F2, F1), jnp.float32, math.log(0.5), math.log(3.0))), 0.5, 3.0)
    weight_rows = normal_values(seeds[4], (HID, OUT), HID ** -0.5, 0.0390625, ((0, 8),))
    target = normal_values(seeds[5], (TOKENS, OUT), 1.0, 6.0, ((0, 4),))
    return dict(activations=activations, left_factor=left_factor, right_factor=right_factor, clip_scale=clip_scale, weight_rows=weight_rows, target=target)


def reference(activations, left_factor, right_factor, clip_scale, weight_rows, target):
    highest = lax.Precision.HIGHEST
    inputs = activations.reshape(TOKENS, F2, F1).astype(jnp.float32)
    mixed = jnp.einsum('tji,ik->tjk', inputs, left_factor, precision=highest)
    rotated = jnp.einsum('jl,tjk->tlk', right_factor, mixed, precision=highest)
    bounded = jnp.tanh(rotated / clip_scale)
    clipped = (clip_scale * bounded).astype(jnp.bfloat16).reshape(TOKENS, HID)
    output = jnp.dot(clipped, weight_rows, preferred_element_type=jnp.float32)
    out_grad = (output - target.astype(jnp.float32)).astype(jnp.bfloat16)
    clipped_grad = lax.dot_general(out_grad, weight_rows, (((1,), (1,)), ((), ())), preferred_element_type=jnp.float32)
    rotated_grad = clipped_grad.reshape(TOKENS, F2, F1) * (1.0 - bounded * bounded)
    mixed_grad = jnp.einsum('jl,tlk->tjk', right_factor, rotated_grad, precision=highest)
    grad_right = jnp.einsum('tjk,tlk->jl', mixed, rotated_grad, precision=highest)
    grad_left = jnp.einsum('tji,tjk->ik', inputs, mixed_grad, precision=highest)
    grad_input = jnp.einsum('tjk,ik->tji', mixed_grad, left_factor, precision=highest).reshape(TOKENS, HID)
    return grad_left, grad_right, grad_input
```

```python
import jax
import jax.numpy as jnp
from jax import lax
from jax.experimental import pallas as pl
from jax.experimental.pallas import tpu as pltpu
from jax.sharding import PartitionSpec as P

BF = jnp.bfloat16
F32 = jnp.float32


def finish_kernel(grad_ref, act_ref, factor_ref, out_ref, left_ref):
    order = factor_ref.shape[0]
    factor = factor_ref[...]

    @pl.when(pl.program_id(0) == 0)
    def _():
        left_ref[...] = jnp.zeros_like(left_ref)

    total = jnp.zeros((order, order), F32)
    for j in range(grad_ref.shape[1] // order):
        here = slice(j * order, (j + 1) * order)
        grad = grad_ref[:, here]
        out_ref[:, here] = lax.dot_general(
            grad, factor, (((1,), (1,)), ((), ())), preferred_element_type=F32
        )
        total = total + lax.dot_general(
            act_ref[:, here], grad, (((0,), (0,)), ((), ())), preferred_element_type=F32
        )
    left_ref[...] += total


def finish(grad, act, factor):
    rows, width = grad.shape
    order = factor.shape[0]
    tile = min(rows, 128)
    return pl.pallas_call(
        finish_kernel,
        grid=(rows // tile,),
        in_specs=[
            pl.BlockSpec((tile, width), lambda i: (i, 0)),
            pl.BlockSpec((tile, width), lambda i: (i, 0)),
            pl.BlockSpec((order, order), lambda i: (0, 0)),
        ],
        out_specs=[
            pl.BlockSpec((tile, width), lambda i: (i, 0)),
            pl.BlockSpec((order, order), lambda i: (0, 0)),
        ],
        out_shape=[
            jax.ShapeDtypeStruct((rows, width), F32),
            jax.ShapeDtypeStruct((order, order), F32),
        ],
        compiler_params=pltpu.CompilerParams(vmem_limit_bytes=48 * 1024 * 1024),
        cost_estimate=pl.CostEstimate(
            flops=4 * rows * width * order, bytes_accessed=8 * rows * width, transcendentals=0
        ),
    )(grad, act, factor.astype(BF))


def split(value):
    head = value.astype(BF)
    return head, (value - head.astype(F32)).astype(BF)


def dot(a, b, dims):
    return lax.dot_general(a, b, ((dims[:1], dims[1:]), ((), ())), preferred_element_type=F32)


MESH = pl.DeviceIdType.MESH


def greet(peers, me):
    barrier = pltpu.get_barrier_semaphore()

    @pl.loop(1, peers)
    def _(o):
        pl.semaphore_signal(
            barrier, inc=1, device_id={"tensor": lax.rem(me + o, peers)}, device_id_type=MESH
        )

    pl.semaphore_wait(barrier, peers - 1)


def to_peer(src, dst, send, recv, peer):
    return pltpu.make_async_remote_copy(
        src_ref=src, dst_ref=dst, send_sem=send, recv_sem=recv,
        device_id={"tensor": peer}, device_id_type=MESH,
    )


def forward_kernel(
    act_ref, left_ref, right_ref, clip_ref,
    out_ref, mixed_ref, bounded_ref,
    in_ref, done_ref, rows_ref, cols_ref,
    in_send, in_recv, out_send, out_recv, own_in, own_out,
):
    peers, chunks, rows, width = act_ref.shape
    order = left_ref.shape[0]
    each = width // order
    me = lax.axis_index("tensor")
    greet(peers, me)

    @pl.loop(0, chunks)
    def _(c):
        pltpu.make_async_copy(act_ref.at[me, c], in_ref.at[me, c], own_in.at[c]).start()

        @pl.loop(1, peers)
        def _(o):
            p = lax.rem(me + o, peers)
            to_peer(
                act_ref.at[p, c], in_ref.at[me, c], in_send.at[c, p], in_recv.at[c, me], p
            ).start()

    left_hi, left_lo = split(left_ref[...])
    right_hi, right_lo = split(right_ref[...])
    clip = clip_ref[...]

    @pl.loop(0, chunks)
    def _(c):
        pltpu.make_async_copy(act_ref.at[me, c], in_ref.at[me, c], own_in.at[c]).wait()

        @pl.loop(1, peers)
        def _(o):
            s = lax.rem(me + o, peers)
            to_peer(
                act_ref.at[s, c], in_ref.at[s, c], in_send.at[c, s], in_recv.at[c, s], s
            ).wait_recv()

        @pl.loop(0, peers)
        def _(s):
            x = jnp.concatenate(
                [in_ref[s, c, :, j * order : (j + 1) * order] for j in range(each)], axis=0
            )
            mixed = dot(x, left_hi, (1, 0)) + dot(x, left_lo, (1, 0))
            for j in range(each):
                rows_ref[s * each + j] = mixed[j * rows : (j + 1) * rows]

        @pl.loop(0, rows, unroll=4)
        def _(t):
            mixed = rows_ref[:, t, :]
            hi, lo = split(mixed)
            mixed_ref[c * rows + t] = hi
            rotated = (
                dot(right_hi, hi, (0, 0)) + dot(right_lo, hi, (0, 0)) + dot(right_hi, lo, (0, 0))
            )
            bounded = jnp.tanh(rotated / clip)
            bounded_ref[c * rows + t] = bounded
            cols_ref[:, t, :] = clip * bounded

        @pl.loop(0, peers)
        def _(s):
            for j in range(each):
                done_ref[s, c, :, j * order : (j + 1) * order] = cols_ref[s * each + j].astype(BF)

        pltpu.make_async_copy(done_ref.at[me, c], out_ref.at[me, c], own_out.at[c]).start()

        @pl.loop(1, peers)
        def _(o):
            p = lax.rem(me + o, peers)
            to_peer(
                done_ref.at[p, c], out_ref.at[me, c], out_send.at[c, p], out_recv.at[c, me], p
            ).start()

    @pl.loop(0, chunks)
    def _(c):
        pltpu.make_async_copy(done_ref.at[me, c], out_ref.at[me, c], own_out.at[c]).wait()

        @pl.loop(1, peers)
        def _(o):
            p = lax.rem(me + o, peers)
            to_peer(
                act_ref.at[p, c], in_ref.at[me, c], in_send.at[c, p], in_recv.at[c, p], p
            ).wait_send()
            to_peer(
                done_ref.at[p, c], out_ref.at[p, c], out_send.at[c, p], out_recv.at[c, p], p
            ).wait()


def forward(act, left, right, clip, rows):
    tok_rows, width = act.shape
    peers = lax.axis_size("tensor")
    own = tok_rows // peers
    chunks = own // rows
    order, side = left.shape[0], right.shape[0]
    blocks = (peers, chunks, rows, width)
    dma = pltpu.SemaphoreType.DMA
    hbm = pl.BlockSpec(memory_space=pl.ANY)
    vmem = pl.BlockSpec(memory_space=pltpu.VMEM)
    out, mixed, bounded = pl.pallas_call(
        forward_kernel,
        out_shape=[
            jax.ShapeDtypeStruct(blocks, BF),
            jax.ShapeDtypeStruct((own, side, order), BF),
            jax.ShapeDtypeStruct((own, side, order), F32),
        ],
        in_specs=[hbm, vmem, vmem, vmem],
        out_specs=[hbm, vmem, vmem],
        scratch_shapes=[
            pltpu.VMEM(blocks, BF), pltpu.VMEM(blocks, BF),
            pltpu.VMEM((side, rows, order), F32), pltpu.VMEM((side, rows, order), F32),
            dma((chunks, peers)), dma((chunks, peers)), dma((chunks, peers)), dma((chunks, peers)),
            dma((chunks,)), dma((chunks,)),
        ],
        compiler_params=pltpu.CompilerParams(
            collective_id=0, has_side_effects=True, vmem_limit_bytes=32 * 1024 * 1024
        ),
    )(act.reshape(blocks), left, right, clip)
    return out.reshape(tok_rows, width), mixed, bounded


def backward_kernel(
    grad_ref, mixed_ref, bounded_ref, right_ref, out_ref, sum_ref, rows_ref, cols_ref
):
    peers, own, width = grad_ref.shape
    order = bounded_ref.shape[2]
    each = width // order
    right = right_ref[...].astype(BF)

    @pl.loop(0, peers)
    def _(s):
        for j in range(each):
            rows_ref[s * each + j] = grad_ref[s, :, j * order : (j + 1) * order].astype(F32)

    sum_ref[...] = jnp.zeros_like(sum_ref)

    @pl.loop(0, own, unroll=4)
    def _(t):
        bounded = bounded_ref[t]
        rotated_grad = (rows_ref[:, t, :] * (1.0 - bounded * bounded)).astype(BF)
        sum_ref[...] += dot(mixed_ref[t], rotated_grad, (1, 1))
        cols_ref[:, t, :] = dot(right, rotated_grad, (1, 0))

    @pl.loop(0, peers)
    def _(s):
        for j in range(each):
            out_ref[s, :, j * order : (j + 1) * order] = cols_ref[s * each + j].astype(BF)


def owner_call(kernel, outs, scratch, *args):
    return pl.pallas_call(
        kernel,
        out_shape=[jax.ShapeDtypeStruct(*out) for out in outs],
        in_specs=[pl.BlockSpec(memory_space=pltpu.VMEM)] * len(args),
        out_specs=[pl.BlockSpec(memory_space=pltpu.VMEM)] * len(outs),
        scratch_shapes=[pltpu.VMEM(scratch, F32)] * 2,
        compiler_params=pltpu.CompilerParams(vmem_limit_bytes=56 * 1024 * 1024),
    )(*args)


def local(activations, left_factor, right_factor, clip_scale, weight_rows, target):
    peers = lax.axis_size("tensor")
    everyone = lax.axis_size("dp") * peers
    tok_rows, width = activations.shape
    width_left = left_factor.shape[0]
    width_right = right_factor.shape[0]
    own = tok_rows // peers

    def exchange(blocks):
        got = lax.all_to_all(
            blocks.reshape(tok_rows, width), "tensor", split_axis=0, concat_axis=0, tiled=True
        )
        return got.reshape(peers, own, width)

    flat = (peers, own, width)
    cube = (own, width_right, width_left)
    by_row = (width_right, own, width_left)
    clipped, mixed, bounded = forward(
        activations, left_factor, right_factor, clip_scale, min(own, 8)
    )
    partial_out = jnp.dot(clipped, weight_rows, preferred_element_type=F32).astype(BF)
    chips = peers // 2
    core = lax.axis_index("tensor") % 2
    same_core = [[2 * q + c for q in range(chips)] for c in range(2)]
    swap = [(d, d ^ 1) for d in range(peers)]
    blocks = partial_out.reshape(chips, 2, own, -1)
    there = lax.dynamic_index_in_dim(blocks, 1 - core, 1, keepdims=False)
    here = lax.dynamic_index_in_dim(blocks, core, 1, keepdims=False)
    there = lax.ppermute(there, "tensor", swap)
    paired = (here.astype(F32) + there.astype(F32)).astype(BF)
    terms = lax.all_to_all(
        paired, "tensor", split_axis=0, concat_axis=0, axis_index_groups=same_core, tiled=True
    )
    total = jnp.sum(terms.astype(F32), axis=0)
    mine = lax.dynamic_slice_in_dim(target, lax.axis_index("tensor") * own, own, 0)
    mine = (total - mine.astype(F32)).astype(BF)
    got = lax.all_to_all(
        jnp.broadcast_to(mine[None], (chips, *mine.shape)),
        "tensor", split_axis=0, concat_axis=0, axis_index_groups=same_core, tiled=True,
    )
    other = lax.ppermute(got, "tensor", swap)
    first = jnp.where(core == 0, got, other)
    second = jnp.where(core == 0, other, got)
    out_grad = jnp.stack([first, second], axis=1).reshape(tok_rows, -1)
    clipped_grad = lax.dot_general(
        out_grad, weight_rows, (((1,), (1,)), ((), ())), preferred_element_type=F32
    ).astype(BF)
    mixed_grad, right_part = owner_call(
        backward_kernel, [(flat, BF), ((width_right, width_right), F32)], by_row,
        exchange(clipped_grad), mixed, bounded, right_factor,
    )
    grad_back = exchange(mixed_grad).reshape(tok_rows, width)
    input_grad, left_part = finish(grad_back, activations, left_factor)

    cols = max(width_left, width_right)
    stacked = jnp.concatenate(
        [
            jnp.pad(left_part, ((0, 0), (0, cols - width_left))),
            jnp.pad(right_part, ((0, 0), (0, cols - width_right))),
        ],
        axis=0,
    )
    rows = -(-stacked.shape[0] // (8 * peers)) * 8
    stacked = jnp.pad(stacked, ((0, rows * peers - stacked.shape[0]), (0, 0)))

    def spread(piece, axis, times):
        copies = jnp.broadcast_to(piece[None], (times, *piece.shape))
        return lax.all_to_all(copies, axis, split_axis=0, concat_axis=0, tiled=True)

    shares = lax.all_to_all(
        stacked.reshape(peers, rows, cols), "tensor", split_axis=0, concat_axis=0, tiled=True
    )
    share = jnp.sum(spread(jnp.sum(shares, axis=0), "dp", lax.axis_size("dp")), axis=0)
    sums = spread(share, "tensor", peers).reshape(rows * peers, cols)
    left_sum = sums[:width_left, :width_left]
    right_sum = sums[width_left : width_left + width_right, :width_right]
    return (left_sum, right_sum, input_grad)


def solution(mesh):
    placed = (P("dp", "tensor"), P(), P(), P(), P("tensor", None), P("dp", None))
    return jax.shard_map(
        local, mesh=mesh, in_specs=placed, out_specs=(P(), P(), P("dp", "tensor")), check_vma=False
    )
```

```python
import jax
import jax.numpy as jnp
from jax import lax
from jax.experimental import pallas as pl
from jax.experimental.pallas import tpu as pltpu
from jax.sharding import PartitionSpec as P

BF = jnp.bfloat16
F32 = jnp.float32
MESH = pl.DeviceIdType.MESH


def split(value):
    head = value.astype(BF)
    return head, (value - head.astype(F32)).astype(BF)


def dot(a, b, dims):
    return lax.dot_general(a, b, ((dims[:1], dims[1:]), ((), ())), preferred_element_type=F32)


def to_peer(src, dst, send, recv, peer):
    return pltpu.make_async_remote_copy(
        src_ref=src, dst_ref=dst, send_sem=send, recv_sem=recv,
        device_id={"tensor": peer}, device_id_type=MESH,
    )


def to_layer(src, dst, send, recv, layer):
    return pltpu.make_async_remote_copy(
        src_ref=src, dst_ref=dst, send_sem=send, recv_sem=recv,
        device_id={"dp": layer}, device_id_type=MESH,
    )


def others(me, count, body):
    @pl.loop(1, count)
    def _(o):
        body(lax.rem(me + o, count))


def kernel(
    act_ref, left_ref, right_ref, clip_ref, weight_ref, target_ref,
    out_ref, sums_ref,
    x_ref, send_ref, recv_ref,
    mixed_ref, slope_ref, rows_ref, cols_ref,
    w_ref, lhs_ref, aim_ref, part_ref, pair_ref, paired_ref, got_ref, grad_ref, acc_ref,
    left_acc, right_acc, stack_ref, shares_ref, layers_ref, total_ref,
    in_send, in_recv, fwd_send, fwd_recv, bwd_send, bwd_recv, end_send, end_recv,
    own_in, own_fwd, own_bwd, own_end, w_sem, aim_sem,
    pair_send, pair_recv, chip_send, chip_recv, all_send, all_recv, relay_send,
    share_send, share_recv, layer_send, layer_recv, sum_send, sum_recv, own_sum,
):
    peers, chunks, rows, width = act_ref.shape
    own = chunks * rows
    order, side = left_ref.shape[0], right_ref.shape[0]
    each = width // order
    blocks, cols = w_ref.shape[0], w_ref.shape[2]
    chips = peers // 2
    layers = layers_ref.shape[0]
    me, layer = lax.axis_index("tensor"), lax.axis_index("dp")
    chip, core = me // 2, lax.rem(me, 2)
    partner = me + 1 - 2 * core

    def act_in(c, p):
        return to_peer(act_ref.at[p, c], x_ref.at[me, c], in_send.at[c, p], in_recv.at[c, me], p)

    def act_got(c, s):
        return to_peer(act_ref.at[s, c], x_ref.at[s, c], in_send.at[c, s], in_recv.at[c, s], s)

    def act_own(c):
        return pltpu.make_async_copy(act_ref.at[me, c], x_ref.at[me, c], own_in.at[c])

    def fwd_out(c, p):
        return to_peer(send_ref.at[p, c], recv_ref.at[me, c], fwd_send.at[c, p], fwd_recv.at[c, me], p)

    def fwd_got(c, s):
        return to_peer(send_ref.at[s, c], recv_ref.at[s, c], fwd_send.at[c, s], fwd_recv.at[c, s], s)

    def fwd_own(c):
        return pltpu.make_async_copy(send_ref.at[me, c], recv_ref.at[me, c], own_fwd.at[c])

    def bwd_out(c, p):
        return to_peer(send_ref.at[p, c], recv_ref.at[me, c], bwd_send.at[c, p], bwd_recv.at[c, me], p)

    def bwd_got(c, s):
        return to_peer(send_ref.at[s, c], recv_ref.at[s, c], bwd_send.at[c, s], bwd_recv.at[c, s], s)

    def bwd_own(c):
        return pltpu.make_async_copy(send_ref.at[me, c], recv_ref.at[me, c], own_bwd.at[c])

    def end_out(c, p):
        return to_peer(send_ref.at[p, c], out_ref.at[me, c], end_send.at[c, p], end_recv.at[c, me], p)

    def end_got(c, s):
        return to_peer(send_ref.at[s, c], out_ref.at[s, c], end_send.at[c, s], end_recv.at[c, s], s)

    def end_own(c):
        return pltpu.make_async_copy(send_ref.at[me, c], out_ref.at[me, c], own_end.at[c])

    def load_w(n):
        here = pl.ds(pl.multiple_of(n * cols, cols), cols)
        return pltpu.make_async_copy(weight_ref.at[:, here], w_ref.at[n], w_sem.at[n])

    def load_aim(n):
        here = pl.ds(pl.multiple_of(n * cols, cols), cols)
        return pltpu.make_async_copy(target_ref.at[me, :, here], aim_ref.at[n], aim_sem.at[n])

    def pair_out(n):
        return to_peer(
            part_ref.at[n, 1 - core], pair_ref.at[n], pair_send.at[n], pair_recv.at[n], partner
        )

    def chip_out(n, q):
        return to_peer(
            paired_ref.at[n, q], got_ref.at[n, chip],
            chip_send.at[n, q], chip_recv.at[n, chip], 2 * q + core,
        )

    def chip_got(n, q):
        return to_peer(
            paired_ref.at[n, q], got_ref.at[n, q],
            chip_send.at[n, q], chip_recv.at[n, q], 2 * q + core,
        )

    def all_out(n, p):
        return to_peer(
            grad_ref.at[n, me], grad_ref.at[n, me], all_send.at[n, p], all_recv.at[n, me], p
        )

    def all_got(n, s):
        return to_peer(
            grad_ref.at[n, s], grad_ref.at[n, s], all_send.at[n, s], all_recv.at[n, s], partner
        )

    def relay(n, q):
        s = 2 * q + core
        return to_peer(
            grad_ref.at[n, s], grad_ref.at[n, s], relay_send.at[n, q], all_recv.at[n, s], partner
        )

    def share_out(p):
        return to_peer(
            stack_ref.at[p], shares_ref.at[me], share_send.at[p], share_recv.at[me], p
        )

    def share_got(s):
        return to_peer(stack_ref.at[s], shares_ref.at[s], share_send.at[s], share_recv.at[s], s)

    def layer_out(d):
        return to_layer(
            layers_ref.at[layer], layers_ref.at[layer], layer_send.at[d], layer_recv.at[layer], d
        )

    def layer_got(d):
        return to_layer(layers_ref.at[d], layers_ref.at[d], layer_send.at[d], layer_recv.at[d], d)

    def sum_out(p):
        return to_peer(total_ref, sums_ref.at[me], sum_send.at[p], sum_recv.at[me], p)

    def sum_got(s):
        return to_peer(total_ref, sums_ref.at[s], sum_send.at[s], sum_recv.at[s], s)

    barrier = pltpu.get_barrier_semaphore()
    others(me, peers, lambda p: pl.semaphore_signal(
        barrier, inc=1, device_id={"tensor": p}, device_id_type=MESH))
    others(layer, layers, lambda d: pl.semaphore_signal(
        barrier, inc=1, device_id={"dp": d}, device_id_type=MESH))
    pl.semaphore_wait(barrier, peers + layers - 2)

    @pl.loop(0, chunks)
    def _(c):
        act_own(c).start()
        others(me, peers, lambda p: act_in(c, p).start())

    @pl.loop(0, blocks)
    def _(n):
        load_w(n).start()
        load_aim(n).start()

    left_hi, left_lo = split(left_ref[...])
    right_hi, right_lo = split(right_ref[...])
    clip = clip_ref[...]

    @pl.loop(0, chunks)
    def _(c):
        act_own(c).wait()
        others(me, peers, lambda s: act_got(c, s).wait_recv())

        @pl.loop(0, peers)
        def _(s):
            x = jnp.concatenate(
                [x_ref[s, c, :, j * order : (j + 1) * order] for j in range(each)], axis=0
            )
            mixed = dot(x, left_hi, (1, 0)) + dot(x, left_lo, (1, 0))
            for j in range(each):
                rows_ref[s * each + j] = mixed[j * rows : (j + 1) * rows]

        @pl.loop(0, rows, unroll=4)
        def _(t):
            mixed = rows_ref[:, t, :]
            hi, lo = split(mixed)
            mixed_ref[c * rows + t] = hi
            rotated = (
                dot(right_hi, hi, (0, 0)) + dot(right_lo, hi, (0, 0)) + dot(right_hi, lo, (0, 0))
            )
            bounded = jnp.tanh(rotated / clip)
            slope_ref[c * rows + t] = (1.0 - bounded * bounded).astype(BF)
            cols_ref[:, t, :] = clip * bounded

        @pl.loop(0, peers)
        def _(s):
            for j in range(each):
                send_ref[s, c, :, j * order : (j + 1) * order] = cols_ref[s * each + j].astype(BF)

        fwd_own(c).start()
        others(me, peers, lambda p: fwd_out(c, p).start())

    @pl.loop(0, chunks)
    def _(c):
        fwd_own(c).wait()
        others(me, peers, lambda s: fwd_got(c, s).wait_recv())

    @pl.loop(0, peers)
    def _(s):
        lhs_ref[s] = jnp.concatenate([recv_ref[s, c] for c in range(chunks)], axis=0)

    acc_ref[...] = jnp.zeros_like(acc_ref)

    def stage(i, lag):
        return pl.when((i >= lag) & (i < blocks + lag))

    @pl.loop(0, blocks + LAGS[4])
    def _(i):
        @stage(i, LAGS[0])
        def _():
            n = i - LAGS[0]
            load_w(n).wait()
            lhs = jnp.concatenate([lhs_ref[s] for s in range(peers)], axis=0)
            full = dot(lhs, w_ref[n], (1, 0))
            for p in range(peers):
                part_ref[n, p % 2, p // 2] = full[p * own : (p + 1) * own].astype(BF)
            pair_out(n).start()

        @stage(i, LAGS[1])
        def _():
            n = i - LAGS[1]
            pair_out(n).wait_recv()
            paired_ref[n] = (part_ref[n, core].astype(F32) + pair_ref[n].astype(F32)).astype(BF)
            others(chip, chips, lambda q: chip_out(n, q).start())

        @stage(i, LAGS[2])
        def _():
            n = i - LAGS[2]
            load_aim(n).wait()
            total = paired_ref[n, chip].astype(F32)
            for o in range(1, chips):
                q = lax.rem(chip + o, chips)
                chip_got(n, q).wait_recv()
                total = total + got_ref[n, q].astype(F32)
            grad_ref[n, me] = (total - aim_ref[n].astype(F32)).astype(BF)
            all_out(n, partner).start()
            others(chip, chips, lambda q: all_out(n, 2 * q + core).start())

        @stage(i, LAGS[3])
        def _():
            n = i - LAGS[3]

            def forward(q):
                all_got(n, 2 * q + core).wait_recv()
                relay(n, q).start()

            others(chip, chips, forward)

        @stage(i, LAGS[4])
        def _():
            n = i - LAGS[4]

            @pl.loop(0, chips)
            def _(q):
                all_got(n, 2 * q + 1 - core).wait_recv()

            grad = jnp.concatenate([grad_ref[n, s] for s in range(peers)], axis=0)
            for h in range(0, width, 512):
                here = slice(h, min(h + 512, width))
                acc_ref[:, here] += dot(grad, w_ref[n, here, :], (1, 1))

    @pl.loop(0, chunks)
    def _(c):
        def drain(p):
            act_in(c, p).wait_send()
            fwd_out(c, p).wait_send()

        others(me, peers, drain)

    @pl.loop(0, chunks)
    def _(c):
        @pl.loop(0, peers)
        def _(p):
            start = pl.multiple_of(p * own + c * rows, rows)
            send_ref[p, c] = acc_ref[pl.ds(start, rows), :].astype(BF)

        bwd_own(c).start()
        others(me, peers, lambda p: bwd_out(c, p).start())

    left_acc[...] = jnp.zeros_like(left_acc)
    right_acc[...] = jnp.zeros_like(right_acc)
    stack_ref[...] = jnp.zeros_like(stack_ref)

    @pl.loop(0, chunks)
    def _(c):
        bwd_own(c).wait()
        others(me, peers, lambda s: bwd_got(c, s).wait_recv())

        @pl.loop(0, peers)
        def _(s):
            for j in range(each):
                rows_ref[s * each + j] = recv_ref[s, c, :, j * order : (j + 1) * order].astype(F32)

        @pl.loop(0, rows, unroll=4)
        def _(t):
            turned = (rows_ref[:, t, :] * slope_ref[c * rows + t].astype(F32)).astype(BF)
            right_acc[...] += dot(mixed_ref[c * rows + t], turned, (1, 1))
            cols_ref[:, t, :] = dot(right_hi, turned, (1, 0))

        def unmixed(s):
            return jnp.concatenate(
                [cols_ref[s * each + j] for j in range(each)], axis=0
            ).astype(BF)

        @pl.loop(0, peers)
        def _(s):
            x = jnp.concatenate(
                [x_ref[s, c, :, j * order : (j + 1) * order] for j in range(each)], axis=0
            )
            left_acc[...] += dot(x, unmixed(s), (0, 0))

        @pl.when(c == chunks - 1)
        def _():
            deep = stack_ref.shape[1]
            half = side // 2
            for g in range(order // 8):
                at = divmod(g * 8, deep)
                stack_ref[at[0], at[1] : at[1] + 8, :order] = left_acc[g * 8 : (g + 1) * 8]
            for g in range(half // 8):
                at = divmod(order + g * 8, deep)
                here = slice(at[1], at[1] + 8)
                stack_ref[at[0], here, :side] = right_acc[g * 8 : (g + 1) * 8]
                stack_ref[at[0], here, side : 2 * side] = right_acc[half + g * 8 : half + (g + 1) * 8]
            others(me, peers, lambda p: share_out(p).start())

        others(me, peers, lambda p: bwd_out(c, p).wait_send())

        @pl.loop(0, peers)
        def _(s):
            grad = dot(unmixed(s), left_hi, (1, 1)).astype(BF)
            for j in range(each):
                send_ref[s, c, :, j * order : (j + 1) * order] = grad[j * rows : (j + 1) * rows]

        end_own(c).start()
        others(me, peers, lambda p: end_out(c, p).start())

    total = stack_ref[me]
    for o in range(1, peers):
        s = lax.rem(me + o, peers)
        share_got(s).wait_recv()
        total = total + shares_ref[s]
    layers_ref[layer] = total
    others(layer, layers, lambda d: layer_out(d).start())
    others(layer, layers, lambda d: layer_got(d).wait_recv())
    total = layers_ref[0]
    for d in range(1, layers):
        total = total + layers_ref[d]
    total_ref[...] = total
    mine = pltpu.make_async_copy(total_ref, sums_ref.at[me], own_sum)
    mine.start()
    others(me, peers, lambda p: sum_out(p).start())

    mine.wait()
    others(layer, layers, lambda d: layer_out(d).wait_send())

    def finish(p):
        share_out(p).wait_send()
        sum_out(p).wait_send()
        sum_got(p).wait_recv()

    others(me, peers, finish)

    @pl.loop(0, chunks)
    def _(c):
        end_own(c).wait()

        def drain(p):
            end_out(c, p).wait_send()
            end_got(c, p).wait_recv()

        others(me, peers, drain)

    @pl.loop(0, blocks)
    def _(n):
        pair_out(n).wait_send()
        all_out(n, partner).wait_send()

        def drain(q):
            chip_out(n, q).wait_send()
            all_out(n, 2 * q + core).wait_send()
            relay(n, q).wait_send()

        others(chip, chips, drain)


LAGS = (0, 1, 3, 5, 6)


def local(activations, left_factor, right_factor, clip_scale, weight_rows, target):
    peers, layers = lax.axis_size("tensor"), lax.axis_size("dp")
    tokens, width = activations.shape
    order, side = left_factor.shape[0], right_factor.shape[0]
    out = weight_rows.shape[1]
    own = tokens // peers
    rows = min(own, 8)
    chunks = own // rows
    chips = peers // 2
    cols = next(b for b in (512, 256, 128) if out % b == 0)
    blocks = out // cols
    lanes = -(-max(order, 2 * side) // 128) * 128
    deep = -(-(order + side // 2) // (8 * peers)) * 8
    flat = (peers, chunks, rows, width)
    cube = (own, side, order)
    by_row = (side, rows, order)
    piece = (peers, deep, lanes)
    dma = pltpu.SemaphoreType.DMA
    hbm = pl.BlockSpec(memory_space=pl.ANY)
    vmem = pl.BlockSpec(memory_space=pltpu.VMEM)
    grid = (chunks, peers)
    scratch = (
        [pltpu.VMEM(flat, BF)] * 3
        + [pltpu.VMEM(cube, BF)] * 2
        + [pltpu.VMEM(by_row, F32)] * 2
        + [
            pltpu.VMEM((blocks, width, cols), BF),
            pltpu.VMEM((peers, own, width), BF),
            pltpu.VMEM((blocks, own, cols), BF),
            pltpu.VMEM((blocks, 2, chips, own, cols), BF),
            pltpu.VMEM((blocks, chips, own, cols), BF),
            pltpu.VMEM((blocks, chips, own, cols), BF),
            pltpu.VMEM((blocks, chips, own, cols), BF),
            pltpu.VMEM((blocks, peers, own, cols), BF),
            pltpu.VMEM((tokens, width), F32),
            pltpu.VMEM((order, order), F32),
            pltpu.VMEM((side, side), F32),
            pltpu.VMEM(piece, F32),
            pltpu.VMEM(piece, F32),
            pltpu.VMEM((layers, deep, lanes), F32),
            pltpu.VMEM((deep, lanes), F32),
        ]
        + [dma(grid)] * 8
        + [dma((chunks,))] * 4
        + [dma((blocks,))] * 4
        + [dma((blocks, chips))] * 2
        + [dma((blocks, peers))] * 2
        + [dma((blocks, chips))]
        + [dma((peers,))] * 2
        + [dma((layers,))] * 2
        + [dma((peers,))] * 2
        + [dma]
    )
    grad, sums = pl.pallas_call(
        kernel,
        out_shape=[jax.ShapeDtypeStruct(flat, BF), jax.ShapeDtypeStruct(piece, F32)],
        in_specs=[hbm, vmem, vmem, vmem, hbm, hbm],
        out_specs=[hbm, hbm],
        scratch_shapes=scratch,
        compiler_params=pltpu.CompilerParams(
            collective_id=0, has_side_effects=True, vmem_limit_bytes=67043328
        ),
    )(
        activations.reshape(flat), left_factor, right_factor, clip_scale,
        weight_rows, target.reshape(peers, own, out),
    )
    sums = sums.reshape(peers * deep, lanes)
    low = sums[order : order + side // 2]
    right_sum = jnp.concatenate([low[:, :side], low[:, side : 2 * side]], axis=0)
    return (sums[:order, :order], right_sum, grad.reshape(tokens, width).astype(F32))


def solution(mesh):
    placed = (P("dp", "tensor"), P(), P(), P(), P("tensor", None), P("dp", None))
    return jax.shard_map(
        local, mesh=mesh, in_specs=placed, out_specs=(P(), P(), P("dp", "tensor")), check_vma=False
    )
```

```python
import jax
import jax.numpy as jnp
from jax import lax
from jax.experimental import pallas as pl
from jax.experimental.pallas import tpu as pltpu
from jax.sharding import PartitionSpec as P

BF = jnp.bfloat16
F32 = jnp.float32
MESH = pl.DeviceIdType.MESH
LAGS = (0, 1, 3, 5, 7, 9, 10)


def split(value):
    head = value.astype(BF)
    return head, (value - head.astype(F32)).astype(BF)


def dot(a, b, dims):
    return lax.dot_general(a, b, ((dims[:1], dims[1:]), ((), ())), preferred_element_type=F32)


def remote(src, dst, send, recv, **where):
    return pltpu.make_async_remote_copy(
        src_ref=src, dst_ref=dst, send_sem=send, recv_sem=recv,
        device_id=where, device_id_type=MESH,
    )


def wait_for(ref, sem):
    pltpu.make_async_copy(ref, ref, sem).wait()


def others(me, count, body):
    @pl.loop(1, count)
    def _(o):
        body(lax.rem(me + o, count))


def kernel(
    act_ref, left_ref, right_ref, clip_ref, weight_ref, target_ref,
    out_ref, sums_ref,
    x_ref, send_ref, recv_ref,
    tall_ref, mixed_ref, slope_ref, rows_ref, cube_ref,
    w_ref, lhs_ref, aim_ref, part_ref, pair_ref, got_ref, last_ref, grad_ref, acc_ref,
    left_acc, right_acc, stack_ref, terms_ref, shares_ref, layers_ref, total_ref,
    in_send, in_recv, fwd_send, fwd_recv, bwd_send, bwd_recv, end_send, end_recv,
    w_sem, aim_sem, pair_send, pair_recv, got_send, got_recv, last_send, last_recv,
    all_send, near_recv, relay_send, far_recv, twins_send, twins_recv,
    share_send, share_recv, layer_send, layer_recv, sum_send, sum_recv,
):
    peers, chunks, rows, width = act_ref.shape
    own = chunks * rows
    order, side = left_ref.shape[0], right_ref.shape[0]
    each = width // order
    blocks, cols = w_ref.shape[0], w_ref.shape[2]
    chips = peers // 2
    layers = layers_ref.shape[0]
    parts, tokens = acc_ref.shape[:2]
    share = tokens // peers
    batch = chunks // parts
    steps = parts * blocks
    wide, high = got_ref.shape[1] + 1, got_ref.shape[2]
    across = wide
    me, layer = lax.axis_index("tensor"), lax.axis_index("dp")
    chip, core = me // 2, lax.rem(me, 2)
    partner = me + 1 - 2 * core
    most = pl.ds(0, peers - 1)

    def unpack(ref, s, c):
        flat = ref[s, c].astype(F32)
        return jnp.concatenate(
            [flat[:, j * order : (j + 1) * order] for j in range(each)], axis=0
        )

    def pack(ref, s, c, value):
        flat = jnp.concatenate(
            [value[j * rows : (j + 1) * rows] for j in range(each)], axis=1
        )
        ref[s, c] = flat.astype(BF)

    def spread(src, dst, send, recv, c):
        pltpu.make_async_copy(src.at[me, c], dst.at[me, c], recv).start()
        others(me, peers, lambda p: remote(
            src.at[p, c], dst.at[me, c], send, recv, tensor=p).start())

    def load_w(n):
        here = pl.ds(pl.multiple_of(n * cols, cols), cols)
        return pltpu.make_async_copy(weight_ref.at[:, here], w_ref.at[n], w_sem.at[n])

    load_aim = pltpu.make_async_copy(target_ref.at[me], aim_ref, aim_sem)

    barrier = pltpu.get_barrier_semaphore()
    others(me, peers, lambda p: pl.semaphore_signal(
        barrier, inc=1, device_id={"tensor": p}, device_id_type=MESH))
    others(layer, layers, lambda d: pl.semaphore_signal(
        barrier, inc=1, device_id={"dp": d}, device_id_type=MESH))
    pl.semaphore_wait(barrier, peers + layers - 2)

    @pl.loop(0, chunks)
    def _(c):
        spread(act_ref, x_ref, in_send, in_recv.at[c], c)

    load_aim.start()

    @pl.loop(0, blocks)
    def _(n):
        load_w(n).start()

    left_hi, left_lo = split(left_ref[...])
    turned_hi, turned_lo = split(jnp.transpose(right_ref[...]))
    turned_wide = jnp.concatenate([turned_hi, turned_hi, turned_lo], axis=1)
    right_hi = right_ref[...].astype(BF)
    clip = jnp.transpose(clip_ref[...])
    unclip = 1.0 / clip

    def forward():
        @pl.loop(0, chunks)
        def _(c):
            wait_for(x_ref.at[:, c], in_recv.at[c])

            @pl.loop(0, peers)
            def _(s):
                x = unpack(x_ref, s, c).astype(BF)
                here = pl.ds(pl.multiple_of(s * each * rows, each * rows), each * rows)
                tall_ref[c, here] = x
                mixed = dot(x, left_hi, (1, 0)) + dot(x, left_lo, (1, 0))
                for j in range(each):
                    rows_ref[s * each + j] = mixed[j * rows : (j + 1) * rows]

            @pl.loop(0, rows, unroll=4)
            def _(t):
                mixed = rows_ref[:, t, :]
                hi, lo = split(mixed)
                mixed_ref[c * rows + t] = hi
                rotated = dot(turned_wide, jnp.concatenate([hi, lo, hi], axis=0), (1, 0))
                bounded = jnp.tanh(rotated * unclip)
                slope_ref[c * rows + t] = (1.0 - bounded * bounded).astype(BF)
                cube_ref[:, t, :] = clip * bounded

            @pl.loop(0, peers)
            def _(s):
                here = pl.ds(pl.multiple_of(s * each, each), each)
                pack(send_ref, s, c, cube_ref[here].reshape(each * rows, order))

            spread(send_ref, recv_ref, fwd_send, fwd_recv.at[c], c)

    def project():
        acc_ref[...] = jnp.zeros_like(acc_ref)
        load_aim.wait()

        def places(n):
            row, col = chip // across, lax.rem(chip, across)
            if across * across != chips:
                return col, row, lambda near, far: far * across + near
            turn = lax.rem(n, 2)

            def at(near, far):
                return (1 - turn) * (far * across + near) + turn * (near * across + far)

            return (1 - turn) * col + turn * row, (1 - turn) * row + turn * col, at

        def stage(i, lag):
            return pl.when((i >= lag) & (i < steps + lag))

        @pl.loop(0, steps + LAGS[6])
        def _(i):
            @stage(i, LAGS[0])
            def _():
                n = i - LAGS[0]
                part, block = n // blocks, lax.rem(n, blocks)

                @pl.when(block == 0)
                def _():
                    for k in range(batch):
                        c = part * batch + k
                        wait_for(recv_ref.at[:, c], fwd_recv.at[c])

                    @pl.loop(0, peers)
                    def _(s):
                        lhs_ref[s] = jnp.concatenate(
                            [recv_ref[s, part * batch + k] for k in range(batch)], axis=0
                        )

                @pl.when(part == 0)
                def _():
                    load_w(block).wait()

                lhs = jnp.concatenate([lhs_ref[s] for s in range(peers)], axis=0)
                full = dot(lhs, w_ref[block], (1, 0))
                for p in range(peers):
                    part_ref[n, p % 2, p // 2] = full[p * share : (p + 1) * share].astype(BF)
                remote(
                    part_ref.at[n, 1 - core], pair_ref.at[n], pair_send, pair_recv.at[n],
                    tensor=partner,
                ).start()

            @stage(i, LAGS[1])
            def _():
                n = i - LAGS[1]
                wait_for(pair_ref.at[n], pair_recv.at[n])
                part_ref[n, core] = (
                    part_ref[n, core].astype(F32) + pair_ref[n].astype(F32)
                ).astype(BF)
                near, far, at = places(n)
                for o in range(1, wide):
                    there = lax.rem(near + o, wide)
                    for k in range(high):
                        remote(
                            part_ref.at[n, core, at(there, k)], got_ref.at[n, o - 1, k],
                            got_send, got_recv.at[n], tensor=2 * at(there, far) + core,
                        ).start()

            @stage(i, LAGS[2])
            def _():
                n = i - LAGS[2]
                near, far, at = places(n)
                wait_for(got_ref.at[n], got_recv.at[n])
                for o in range(1, high):
                    there = lax.rem(far + o, high)
                    block = part_ref.at[n, core, at(near, there)]
                    total = block[...].astype(F32)
                    for k in range(wide - 1):
                        total = total + got_ref[n, k, there].astype(F32)
                    block[...] = total.astype(BF)
                    remote(
                        block, last_ref.at[n, o - 1], last_send, last_recv.at[n],
                        tensor=2 * at(near, there) + core,
                    ).start()

            @stage(i, LAGS[3])
            def _():
                n = i - LAGS[3]
                near, far, at = places(n)
                wait_for(last_ref.at[n], last_recv.at[n])
                total = part_ref[n, core, chip].astype(F32)
                for k in range(wide - 1):
                    total = total + got_ref[n, k, far].astype(F32)
                for k in range(high - 1):
                    total = total + last_ref[n, k].astype(F32)
                part, block = n // blocks, lax.rem(n, blocks)
                here = pl.ds(pl.multiple_of(block * cols, cols), cols)
                aim = aim_ref[pl.ds(pl.multiple_of(part * share, share), share), here]
                grad_ref[n, me] = (total - aim.astype(F32)).astype(BF)
                mine = grad_ref.at[n, me]
                for o in range(1, wide):
                    remote(
                        mine, mine, all_send, near_recv.at[n],
                        tensor=2 * at(lax.rem(near + o, wide), far) + core,
                    ).start()
                for o in range(1, high):
                    remote(
                        mine, mine, all_send, far_recv.at[n],
                        tensor=2 * at(near, lax.rem(far + o, high)) + core,
                    ).start()
                remote(mine, mine, all_send, twins_recv.at[n], tensor=partner).start()

            @stage(i, LAGS[4])
            def _():
                n = i - LAGS[4]
                near, far, at = places(n)
                wait_for(grad_ref.at[n, pl.ds(0, wide - 1)], near_recv.at[n])
                for o in range(1, wide):
                    block = grad_ref.at[n, 2 * at(lax.rem(near + o, wide), far) + core]
                    for k in range(1, high):
                        remote(
                            block, block, relay_send, far_recv.at[n],
                            tensor=2 * at(near, lax.rem(far + k, high)) + core,
                        ).start()
                    remote(block, block, twins_send, twins_recv.at[n], tensor=partner).start()

            @stage(i, LAGS[5])
            def _():
                n = i - LAGS[5]
                near, far, at = places(n)
                wait_for(grad_ref.at[n, pl.ds(0, (high - 1) * wide)], far_recv.at[n])
                for o in range(1, high):
                    for k in range(wide):
                        block = grad_ref.at[n, 2 * at(k, lax.rem(far + o, high)) + core]
                        remote(block, block, twins_send, twins_recv.at[n], tensor=partner).start()

            @stage(i, LAGS[6])
            def _():
                n = i - LAGS[6]
                wait_for(grad_ref.at[n, pl.ds(0, chips)], twins_recv.at[n])
                part, block = n // blocks, lax.rem(n, blocks)
                grad = jnp.concatenate([grad_ref[n, s] for s in range(peers)], axis=0)
                for h in range(0, width, 512):
                    here = slice(h, min(h + 512, width))
                    acc_ref[part, :, here] += dot(grad, w_ref[block, here, :], (1, 1))

                @pl.when(n == blocks - 1)
                def _():
                    wait_for(send_ref.at[most], fwd_send)

                @pl.when(block == blocks - 1)
                def _():
                    for k in range(batch):
                        c = part * batch + k

                        @pl.loop(0, peers)
                        def _(p):
                            start = pl.multiple_of(p * share + k * rows, rows)
                            send_ref[p, c] = acc_ref[part, pl.ds(start, rows), :].astype(BF)

                        spread(send_ref, recv_ref, bwd_send.at[c], bwd_recv.at[c], c)

    def drain_forward():
        wait_for(x_ref.at[most], in_send)

    def backward():
        left_acc[...] = jnp.zeros_like(left_acc)
        right_acc[...] = jnp.zeros_like(right_acc)
        stack_ref[...] = jnp.zeros_like(stack_ref)

        @pl.loop(0, chunks)
        def _(c):
            wait_for(recv_ref.at[:, c], bwd_recv.at[c])

            @pl.loop(0, peers)
            def _(s):
                here = pl.ds(pl.multiple_of(s * each, each), each)
                rows_ref[here] = unpack(recv_ref, s, c).reshape(each, rows, order)

            @pl.loop(0, rows, unroll=4)
            def _(t):
                turned = (rows_ref[:, t, :] * slope_ref[c * rows + t].astype(F32)).astype(BF)
                right_acc[...] += dot(mixed_ref[c * rows + t], turned, (1, 1))
                cube_ref[:, t, :] = dot(right_hi, turned, (1, 0))

            unmixed = cube_ref[...].reshape(side * rows, order).astype(BF)
            left_acc[...] += dot(tall_ref[c], unmixed, (0, 0))

            @pl.when(c == chunks - 1)
            def _():
                deep = stack_ref.shape[1]
                half = side // 2
                for g in range(order // 8):
                    p, at = divmod(g * 8, deep)
                    stack_ref[p, at : at + 8, :order] = left_acc[g * 8 : (g + 1) * 8]
                for g in range(half // 8):
                    p, at = divmod(order + g * 8, deep)
                    top = right_acc[g * 8 : (g + 1) * 8]
                    low = right_acc[half + g * 8 : half + (g + 1) * 8]
                    stack_ref[p, at : at + 8, :side] = top
                    stack_ref[p, at : at + 8, side : 2 * side] = low
                terms_ref[...] = stack_ref[...].astype(BF)
                for o in range(1, peers):
                    p = lax.rem(me + o, peers)
                    remote(
                        terms_ref.at[p], shares_ref.at[o - 1], share_send, share_recv, tensor=p
                    ).start()

            wait_for(send_ref.at[most, c], bwd_send.at[c])

            @pl.loop(0, peers)
            def _(s):
                here = pl.ds(pl.multiple_of(s * each, each), each)
                unmixed = cube_ref[here].reshape(each * rows, order).astype(BF)
                pack(send_ref, s, c, dot(unmixed, left_hi, (1, 1)))

            spread(send_ref, out_ref, end_send, end_recv, c)

    def combine():
        wait_for(shares_ref.at[most], share_recv)
        total = stack_ref[me]
        for o in range(1, peers):
            total = total + shares_ref[o - 1].astype(F32)
        layers_ref[layer] = total
        mine = layers_ref.at[layer]
        others(layer, layers, lambda d: remote(
            mine, mine, layer_send, layer_recv, dp=d).start())
        wait_for(layers_ref.at[pl.ds(0, layers - 1)], layer_recv)
        total = layers_ref[0]
        for d in range(1, layers):
            total = total + layers_ref[d]
        total_ref[...] = total.astype(BF)
        pltpu.make_async_copy(total_ref, sums_ref.at[me], sum_recv).start()
        others(me, peers, lambda p: remote(
            total_ref, sums_ref.at[me], sum_send, sum_recv, tensor=p).start())

        wait_for(sums_ref, sum_recv)
        wait_for(layers_ref.at[pl.ds(0, layers - 1)], layer_send)
        wait_for(shares_ref.at[most], share_send)
        wait_for(shares_ref.at[most], sum_send)

    def drain_ends():
        wait_for(out_ref, end_recv)
        wait_for(send_ref.at[most], end_send)

    def drain_blocks():
        wait_for(part_ref.at[:, 0], pair_send)
        wait_for(got_ref, got_send)
        wait_for(last_ref, last_send)
        wait_for(grad_ref.at[:, pl.ds(0, wide + high - 1)], all_send)
        wait_for(grad_ref.at[:, pl.ds(0, (wide - 1) * (high - 1))], relay_send)
        wait_for(grad_ref.at[:, pl.ds(0, chips - 1)], twins_send)

    forward()
    project()
    drain_forward()
    backward()
    combine()
    drain_ends()
    drain_blocks()


def finish_kernel(
    grad_ref, sums_ref, out_ref, left_ref, right_ref, in_buf, out_buf, in_sem, out_sem
):
    steps = in_buf.shape[0]

    def load(i):
        return pltpu.make_async_copy(grad_ref.at[i], in_buf.at[i], in_sem.at[i])

    def store(i):
        return pltpu.make_async_copy(out_buf.at[i], out_ref.at[i], out_sem.at[i])

    for i in range(steps):
        load(i).start()
    order, side = left_ref.shape[0], right_ref.shape[0]
    half = side // 2
    left_ref[...] = sums_ref[:order, :order].astype(F32)
    right_ref[:half] = sums_ref[order : order + half, :side].astype(F32)
    right_ref[half:] = sums_ref[order : order + half, side : 2 * side].astype(F32)
    for i in range(steps):
        load(i).wait()
        out_buf[i] = in_buf[i].astype(F32)
        store(i).start()
    for i in range(steps):
        store(i).wait()


def finish(grad, sums, order, side):
    tokens, width = grad.shape
    steps = tokens // 32
    split_up = (steps, 32, width)
    hbm = pl.BlockSpec(memory_space=pl.ANY)
    vmem = pl.BlockSpec(memory_space=pltpu.VMEM)
    out, left, right = pl.pallas_call(
        finish_kernel,
        in_specs=[hbm, vmem],
        out_specs=[hbm, vmem, vmem],
        out_shape=[
            jax.ShapeDtypeStruct(split_up, F32),
            jax.ShapeDtypeStruct((order, order), F32),
            jax.ShapeDtypeStruct((side, side), F32),
        ],
        scratch_shapes=[
            pltpu.VMEM(split_up, BF),
            pltpu.VMEM(split_up, F32),
            pltpu.SemaphoreType.DMA((steps,)),
            pltpu.SemaphoreType.DMA((steps,)),
        ],
    )(grad.reshape(split_up), sums)
    return out.reshape(tokens, width), left, right


def local(activations, left_factor, right_factor, clip_scale, weight_rows, target):
    peers, layers = lax.axis_size("tensor"), lax.axis_size("dp")
    tokens, width = activations.shape
    order, side = left_factor.shape[0], right_factor.shape[0]
    out = weight_rows.shape[1]
    own = tokens // peers
    rows = min(own, 8)
    chunks = own // rows
    chips = peers // 2
    across = max(b for b in range(1, chips + 1) if chips % b == 0 and b * b <= chips)
    across = chips // across
    cols = next(b for b in (512, 256, 128) if out % b == 0)
    blocks = out // cols
    parts = 1
    steps, share = parts * blocks, own // parts
    lanes = -(-max(order, 2 * side) // 128) * 128
    deep = -(-(order + side // 2) // (8 * peers)) * 8
    flat = (peers, chunks, rows, width)
    cube = (own, side, order)
    piece = (peers, deep, lanes)
    dma = pltpu.SemaphoreType.DMA
    hbm = pl.BlockSpec(memory_space=pl.ANY)
    vmem = pl.BlockSpec(memory_space=pltpu.VMEM)
    scratch = (
        [pltpu.VMEM(flat, BF)] * 3
        + [pltpu.VMEM((chunks, side * rows, order), BF)]
        + [pltpu.VMEM(cube, BF)] * 2
        + [
            pltpu.VMEM((side, rows, order), F32),
            pltpu.VMEM((side, rows, order), F32),
            pltpu.VMEM((blocks, width, cols), BF),
            pltpu.VMEM((peers, share, width), BF),
            pltpu.VMEM((own, out), BF),
            pltpu.VMEM((steps, 2, chips, share, cols), BF),
            pltpu.VMEM((steps, chips, share, cols), BF),
            pltpu.VMEM((steps, across - 1, chips // across, share, cols), BF),
            pltpu.VMEM((steps, chips // across - 1, share, cols), BF),
            pltpu.VMEM((steps, peers, share, cols), BF),
            pltpu.VMEM((parts, tokens // parts, width), F32),
            pltpu.VMEM((order, order), F32),
            pltpu.VMEM((side, side), F32),
            pltpu.VMEM(piece, F32),
            pltpu.VMEM(piece, BF),
            pltpu.VMEM(piece, BF),
            pltpu.VMEM((layers, deep, lanes), F32),
            pltpu.VMEM((deep, lanes), BF),
        ]
        + [dma, dma((chunks,))] * 2
        + [dma((chunks,))] * 2
        + [dma] * 2
        + [dma((blocks,)), dma]
        + [dma, dma((steps,))] * 6
        + [dma] * 6
    )
    grad, sums = pl.pallas_call(
        kernel,
        out_shape=[jax.ShapeDtypeStruct(flat, BF), jax.ShapeDtypeStruct(piece, BF)],
        in_specs=[hbm, vmem, vmem, vmem, hbm, hbm],
        out_specs=[hbm, hbm],
        scratch_shapes=scratch,
        compiler_params=pltpu.CompilerParams(
            collective_id=0, has_side_effects=True, vmem_limit_bytes=67043328
        ),
    )(
        activations.reshape(flat), left_factor, right_factor, clip_scale.T,
        weight_rows, target.reshape(peers, own, out),
    )
    input_grad, left_sum, right_sum = finish(
        grad.reshape(tokens, width), sums.reshape(peers * deep, lanes), order, side
    )
    return (left_sum, right_sum, input_grad)


def solution(mesh):
    placed = (P("dp", "tensor"), P(), P(), P(), P("tensor", None), P("dp", None))
    return jax.shard_map(
        local, mesh=mesh, in_specs=placed, out_specs=(P(), P(), P("dp", "tensor")), check_vma=False
    )
```

```python
import jax
import jax.numpy as jnp
from jax import lax
from jax.experimental import pallas as pl
from jax.experimental.pallas import tpu as pltpu
from jax.sharding import PartitionSpec as P

BF = jnp.bfloat16
F32 = jnp.float32
MESH = pl.DeviceIdType.MESH
LAGS = (0, 1, 3, 5, 7, 9, 10)


def split(value):
    head = value.astype(BF)
    return head, (value - head.astype(F32)).astype(BF)


def dot(a, b, dims):
    return lax.dot_general(a, b, ((dims[:1], dims[1:]), ((), ())), preferred_element_type=F32)


def remote(src, dst, send, recv, **where):
    return pltpu.make_async_remote_copy(
        src_ref=src, dst_ref=dst, send_sem=send, recv_sem=recv,
        device_id=where, device_id_type=MESH,
    )


def wait_for(ref, sem):
    pltpu.make_async_copy(ref, ref, sem).wait()


def others(me, count, body):
    @pl.loop(1, count)
    def _(o):
        body(lax.rem(me + o, count))


def kernel(
    act_ref, left_ref, right_ref, clip_ref, weight_ref, target_ref,
    out_ref, sums_ref,
    x_ref, send_ref, recv_ref,
    tall_ref, mixed_ref, slope_ref, rows_ref, cube_ref,
    w_ref, lhs_ref, aim_ref, part_ref, pair_ref, got_ref, last_ref, grad_ref, acc_ref,
    left_acc, right_acc, stack_ref, terms_ref, shares_ref, layers_ref, total_ref,
    in_send, in_recv, fwd_send, fwd_recv, bwd_send, bwd_recv, end_send, end_recv,
    w_sem, aim_sem, pair_send, pair_recv, got_send, got_recv, last_send, last_recv,
    all_send, near_recv, relay_send, far_recv, twins_send, twins_recv,
    share_send, share_recv, layer_send, layer_recv, sum_send, sum_recv,
):
    peers, chunks, rows, width = act_ref.shape
    own = chunks * rows
    order, side = left_ref.shape[0], right_ref.shape[0]
    each = width // order
    blocks, cols = w_ref.shape[0], w_ref.shape[2]
    chips = peers // 2
    layers = layers_ref.shape[0]
    parts, tokens = acc_ref.shape[:2]
    share = tokens // peers
    batch = chunks // parts
    steps = parts * blocks
    wide, high = got_ref.shape[1] + 1, got_ref.shape[2]
    across = wide
    me, layer = lax.axis_index("tensor"), lax.axis_index("dp")
    chip, core = me // 2, lax.rem(me, 2)
    partner = me + 1 - 2 * core
    most = pl.ds(0, peers - 1)

    def unpack(ref, s, c):
        flat = ref[s, c].astype(F32)
        return jnp.concatenate(
            [flat[:, j * order : (j + 1) * order] for j in range(each)], axis=0
        )

    def pack(ref, s, c, value):
        flat = jnp.concatenate(
            [value[j * rows : (j + 1) * rows] for j in range(each)], axis=1
        )
        ref[s, c] = flat.astype(BF)

    def spread(src, dst, send, recv, c):
        pltpu.make_async_copy(src.at[me, c], dst.at[me, c], recv).start()
        others(me, peers, lambda p: remote(
            src.at[p, c], dst.at[me, c], send, recv, tensor=p).start())

    def load_w(n):
        here = pl.ds(pl.multiple_of(n * cols, cols), cols)
        return pltpu.make_async_copy(weight_ref.at[:, here], w_ref.at[n], w_sem.at[n])

    load_aim = pltpu.make_async_copy(target_ref.at[me], aim_ref, aim_sem)

    barrier = pltpu.get_barrier_semaphore()
    others(me, peers, lambda p: pl.semaphore_signal(
        barrier, inc=1, device_id={"tensor": p}, device_id_type=MESH))
    others(layer, layers, lambda d: pl.semaphore_signal(
        barrier, inc=1, device_id={"dp": d}, device_id_type=MESH))
    pl.semaphore_wait(barrier, peers + layers - 2)

    @pl.loop(0, chunks)
    def _(c):
        spread(act_ref, x_ref, in_send, in_recv.at[c], c)

    load_aim.start()

    @pl.loop(0, blocks)
    def _(n):
        load_w(n).start()

    left_hi, left_lo = split(left_ref[...])
    turned_hi, turned_lo = split(jnp.transpose(right_ref[...]))
    turned_wide = jnp.concatenate([turned_hi, turned_hi, turned_lo], axis=1)
    right_hi = right_ref[...].astype(BF)
    clip = jnp.transpose(clip_ref[...])
    unclip = 1.0 / clip

    def forward():
        @pl.loop(0, chunks)
        def _(c):
            wait_for(x_ref.at[:, c], in_recv.at[c])

            @pl.loop(0, peers)
            def _(s):
                x = unpack(x_ref, s, c).astype(BF)
                here = pl.ds(pl.multiple_of(s * each * rows, each * rows), each * rows)
                tall_ref[c, here] = x
                mixed = dot(x, left_hi, (1, 0)) + dot(x, left_lo, (1, 0))
                for j in range(each):
                    rows_ref[s * each + j] = mixed[j * rows : (j + 1) * rows]

            @pl.loop(0, rows, unroll=4)
            def _(t):
                mixed = rows_ref[:, t, :]
                hi, lo = split(mixed)
                mixed_ref[c * rows + t] = hi
                rotated = dot(turned_wide, jnp.concatenate([hi, lo, hi], axis=0), (1, 0))
                bounded = jnp.tanh(rotated * unclip)
                slope_ref[c * rows + t] = (1.0 - bounded * bounded).astype(BF)
                cube_ref[:, t, :] = clip * bounded

            @pl.loop(0, peers)
            def _(s):
                here = pl.ds(pl.multiple_of(s * each, each), each)
                pack(send_ref, s, c, cube_ref[here].reshape(each * rows, order))

            spread(send_ref, recv_ref, fwd_send, fwd_recv.at[c], c)

    def project():
        acc_ref[...] = jnp.zeros_like(acc_ref)
        load_aim.wait()

        def places(n):
            row, col = chip // across, lax.rem(chip, across)
            if across * across != chips:
                return col, row, lambda near, far: far * across + near
            turn = lax.rem(n, 2)

            def at(near, far):
                return (1 - turn) * (far * across + near) + turn * (near * across + far)

            return (1 - turn) * col + turn * row, (1 - turn) * row + turn * col, at

        def stage(i, lag):
            return pl.when((i >= lag) & (i < steps + lag))

        @pl.loop(0, steps + LAGS[6])
        def _(i):
            @stage(i, LAGS[0])
            def _():
                n = i - LAGS[0]
                part, block = n // blocks, lax.rem(n, blocks)

                @pl.when(block == 0)
                def _():
                    for k in range(batch):
                        c = part * batch + k
                        wait_for(recv_ref.at[:, c], fwd_recv.at[c])

                    @pl.loop(0, peers)
                    def _(s):
                        lhs_ref[s] = jnp.concatenate(
                            [recv_ref[s, part * batch + k] for k in range(batch)], axis=0
                        )

                @pl.when(part == 0)
                def _():
                    load_w(block).wait()

                lhs = jnp.concatenate([lhs_ref[s] for s in range(peers)], axis=0)
                full = dot(lhs, w_ref[block], (1, 0))
                for p in range(peers):
                    part_ref[n, p % 2, p // 2] = full[p * share : (p + 1) * share].astype(BF)
                remote(
                    part_ref.at[n, 1 - core], pair_ref.at[n], pair_send, pair_recv.at[n],
                    tensor=partner,
                ).start()

            @stage(i, LAGS[1])
            def _():
                n = i - LAGS[1]
                wait_for(pair_ref.at[n], pair_recv.at[n])
                part_ref[n, core] = (
                    part_ref[n, core].astype(F32) + pair_ref[n].astype(F32)
                ).astype(BF)
                near, far, at = places(n)
                for o in range(1, wide):
                    there = lax.rem(near + o, wide)
                    for k in range(high):
                        remote(
                            part_ref.at[n, core, at(there, k)], got_ref.at[n, o - 1, k],
                            got_send, got_recv.at[n], tensor=2 * at(there, far) + core,
                        ).start()

            @stage(i, LAGS[2])
            def _():
                n = i - LAGS[2]
                near, far, at = places(n)
                wait_for(got_ref.at[n], got_recv.at[n])
                for o in range(1, high):
                    there = lax.rem(far + o, high)
                    block = part_ref.at[n, core, at(near, there)]
                    total = block[...].astype(F32)
                    for k in range(wide - 1):
                        total = total + got_ref[n, k, there].astype(F32)
                    block[...] = total.astype(BF)
                    remote(
                        block, last_ref.at[n, o - 1], last_send, last_recv.at[n],
                        tensor=2 * at(near, there) + core,
                    ).start()

            @stage(i, LAGS[3])
            def _():
                n = i - LAGS[3]
                near, far, at = places(n)
                wait_for(last_ref.at[n], last_recv.at[n])
                total = part_ref[n, core, chip].astype(F32)
                for k in range(wide - 1):
                    total = total + got_ref[n, k, far].astype(F32)
                for k in range(high - 1):
                    total = total + last_ref[n, k].astype(F32)
                part, block = n // blocks, lax.rem(n, blocks)
                here = pl.ds(pl.multiple_of(block * cols, cols), cols)
                aim = aim_ref[pl.ds(pl.multiple_of(part * share, share), share), here]
                grad_ref[n, me] = (total - aim.astype(F32)).astype(BF)
                mine = grad_ref.at[n, me]
                for o in range(1, wide):
                    remote(
                        mine, mine, all_send, near_recv.at[n],
                        tensor=2 * at(lax.rem(near + o, wide), far) + core,
                    ).start()
                for o in range(1, high):
                    remote(
                        mine, mine, all_send, far_recv.at[n],
                        tensor=2 * at(near, lax.rem(far + o, high)) + core,
                    ).start()
                remote(mine, mine, all_send, twins_recv.at[n], tensor=partner).start()

            @stage(i, LAGS[4])
            def _():
                n = i - LAGS[4]
                near, far, at = places(n)
                wait_for(grad_ref.at[n, pl.ds(0, wide - 1)], near_recv.at[n])
                for o in range(1, wide):
                    block = grad_ref.at[n, 2 * at(lax.rem(near + o, wide), far) + core]
                    for k in range(1, high):
                        remote(
                            block, block, relay_send, far_recv.at[n],
                            tensor=2 * at(near, lax.rem(far + k, high)) + core,
                        ).start()
                    remote(block, block, twins_send, twins_recv.at[n], tensor=partner).start()

            @stage(i, LAGS[5])
            def _():
                n = i - LAGS[5]
                near, far, at = places(n)
                wait_for(grad_ref.at[n, pl.ds(0, (high - 1) * wide)], far_recv.at[n])
                for o in range(1, high):
                    for k in range(wide):
                        block = grad_ref.at[n, 2 * at(k, lax.rem(far + o, high)) + core]
                        remote(block, block, twins_send, twins_recv.at[n], tensor=partner).start()

            @stage(i, LAGS[6])
            def _():
                n = i - LAGS[6]
                wait_for(grad_ref.at[n, pl.ds(0, chips)], twins_recv.at[n])
                part, block = n // blocks, lax.rem(n, blocks)
                grad = jnp.concatenate([grad_ref[n, s] for s in range(peers)], axis=0)
                for h in range(0, width, 512):
                    here = slice(h, min(h + 512, width))
                    acc_ref[part, :, here] += dot(grad, w_ref[block, here, :], (1, 1))

                @pl.when(n == blocks - 1)
                def _():
                    wait_for(send_ref.at[most], fwd_send)

                @pl.when(block == blocks - 1)
                def _():
                    for k in range(batch):
                        c = part * batch + k

                        @pl.loop(0, peers)
                        def _(p):
                            start = pl.multiple_of(p * share + k * rows, rows)
                            send_ref[p, c] = acc_ref[part, pl.ds(start, rows), :].astype(BF)

                        spread(send_ref, recv_ref, bwd_send.at[c], bwd_recv.at[c], c)

    def drain_forward():
        wait_for(x_ref.at[most], in_send)

    def backward():
        left_acc[...] = jnp.zeros_like(left_acc)
        right_acc[...] = jnp.zeros_like(right_acc)
        stack_ref[...] = jnp.zeros_like(stack_ref)

        @pl.loop(0, chunks)
        def _(c):
            wait_for(recv_ref.at[:, c], bwd_recv.at[c])

            @pl.loop(0, peers)
            def _(s):
                here = pl.ds(pl.multiple_of(s * each, each), each)
                rows_ref[here] = unpack(recv_ref, s, c).reshape(each, rows, order)

            @pl.loop(0, rows, unroll=4)
            def _(t):
                turned = (rows_ref[:, t, :] * slope_ref[c * rows + t].astype(F32)).astype(BF)
                right_acc[...] += dot(mixed_ref[c * rows + t], turned, (1, 1))
                cube_ref[:, t, :] = dot(right_hi, turned, (1, 0))

            unmixed = cube_ref[...].reshape(side * rows, order).astype(BF)
            left_acc[...] += dot(tall_ref[c], unmixed, (0, 0))

            @pl.when(c == chunks - 1)
            def _():
                deep = stack_ref.shape[1]
                half = side // 2
                for g in range(order // 8):
                    p, at = divmod(g * 8, deep)
                    stack_ref[p, at : at + 8, :order] = left_acc[g * 8 : (g + 1) * 8]
                for g in range(half // 8):
                    p, at = divmod(order + g * 8, deep)
                    top = right_acc[g * 8 : (g + 1) * 8]
                    low = right_acc[half + g * 8 : half + (g + 1) * 8]
                    stack_ref[p, at : at + 8, :side] = top
                    stack_ref[p, at : at + 8, side : 2 * side] = low
                terms_ref[...] = stack_ref[...].astype(BF)
                for o in range(1, peers):
                    p = lax.rem(me + o, peers)
                    remote(
                        terms_ref.at[p], shares_ref.at[o - 1], share_send, share_recv, tensor=p
                    ).start()

                @pl.loop(1, chunks - 1)
                def _(k):
                    spread(send_ref, out_ref, end_send, end_recv, k)

            wait_for(send_ref.at[most, c], bwd_send.at[c])

            @pl.loop(0, peers)
            def _(s):
                here = pl.ds(pl.multiple_of(s * each, each), each)
                unmixed = cube_ref[here].reshape(each * rows, order).astype(BF)
                pack(send_ref, s, c, dot(unmixed, left_hi, (1, 1)))

            if chunks > 1:

                @pl.when(c == 0)
                def _():
                    spread(send_ref, out_ref, end_send, end_recv, c)

    def combine():
        wait_for(shares_ref.at[most], share_recv)
        total = stack_ref[me]
        for o in range(1, peers):
            total = total + shares_ref[o - 1].astype(F32)
        layers_ref[layer] = total
        mine = layers_ref.at[layer]
        others(layer, layers, lambda d: remote(
            mine, mine, layer_send, layer_recv, dp=d).start())
        wait_for(layers_ref.at[pl.ds(0, layers - 1)], layer_recv)
        total = layers_ref[0]
        for d in range(1, layers):
            total = total + layers_ref[d]
        total_ref[...] = total.astype(BF)
        pltpu.make_async_copy(total_ref, sums_ref.at[me], sum_recv).start()
        others(me, peers, lambda p: remote(
            total_ref, sums_ref.at[me], sum_send, sum_recv, tensor=p).start())
        spread(send_ref, out_ref, end_send, end_recv, chunks - 1)

        wait_for(sums_ref, sum_recv)
        wait_for(layers_ref.at[pl.ds(0, layers - 1)], layer_send)
        wait_for(shares_ref.at[most], share_send)
        wait_for(shares_ref.at[most], sum_send)

    def drain_ends():
        wait_for(out_ref, end_recv)
        wait_for(send_ref.at[most], end_send)

    def drain_blocks():
        wait_for(part_ref.at[:, 0], pair_send)
        wait_for(got_ref, got_send)
        wait_for(last_ref, last_send)
        wait_for(grad_ref.at[:, pl.ds(0, wide + high - 1)], all_send)
        wait_for(grad_ref.at[:, pl.ds(0, (wide - 1) * (high - 1))], relay_send)
        wait_for(grad_ref.at[:, pl.ds(0, chips - 1)], twins_send)

    forward()
    project()
    drain_forward()
    backward()
    combine()
    drain_ends()
    drain_blocks()


def finish_kernel(
    grad_ref, sums_ref, out_ref, left_ref, right_ref, in_buf, out_buf, in_sem, out_sem
):
    steps = in_buf.shape[0]

    def load(i):
        return pltpu.make_async_copy(grad_ref.at[i], in_buf.at[i], in_sem.at[i])

    def store(i):
        return pltpu.make_async_copy(out_buf.at[i], out_ref.at[i], out_sem.at[i])

    for i in range(steps):
        load(i).start()
    order, side = left_ref.shape[0], right_ref.shape[0]
    half = side // 2
    left_ref[...] = sums_ref[:order, :order].astype(F32)
    right_ref[:half] = sums_ref[order : order + half, :side].astype(F32)
    right_ref[half:] = sums_ref[order : order + half, side : 2 * side].astype(F32)
    for i in range(steps):
        load(i).wait()
        out_buf[i] = in_buf[i].astype(F32)
        store(i).start()
    for i in range(steps):
        store(i).wait()


def finish(grad, sums, order, side):
    tokens, width = grad.shape
    steps = tokens // 32
    split_up = (steps, 32, width)
    hbm = pl.BlockSpec(memory_space=pl.ANY)
    vmem = pl.BlockSpec(memory_space=pltpu.VMEM)
    out, left, right = pl.pallas_call(
        finish_kernel,
        in_specs=[hbm, vmem],
        out_specs=[hbm, vmem, vmem],
        out_shape=[
            jax.ShapeDtypeStruct(split_up, F32),
            jax.ShapeDtypeStruct((order, order), F32),
            jax.ShapeDtypeStruct((side, side), F32),
        ],
        scratch_shapes=[
            pltpu.VMEM(split_up, BF),
            pltpu.VMEM(split_up, F32),
            pltpu.SemaphoreType.DMA((steps,)),
            pltpu.SemaphoreType.DMA((steps,)),
        ],
    )(grad.reshape(split_up), sums)
    return out.reshape(tokens, width), left, right


def local(activations, left_factor, right_factor, clip_scale, weight_rows, target):
    peers, layers = lax.axis_size("tensor"), lax.axis_size("dp")
    tokens, width = activations.shape
    order, side = left_factor.shape[0], right_factor.shape[0]
    out = weight_rows.shape[1]
    own = tokens // peers
    rows = min(own, 8)
    chunks = own // rows
    chips = peers // 2
    across = max(b for b in range(1, chips + 1) if chips % b == 0 and b * b <= chips)
    across = chips // across
    cols = next(b for b in (512, 256, 128) if out % b == 0)
    blocks = out // cols
    parts = 1
    steps, share = parts * blocks, own // parts
    lanes = -(-max(order, 2 * side) // 128) * 128
    deep = -(-(order + side // 2) // (8 * peers)) * 8
    flat = (peers, chunks, rows, width)
    cube = (own, side, order)
    piece = (peers, deep, lanes)
    dma = pltpu.SemaphoreType.DMA
    hbm = pl.BlockSpec(memory_space=pl.ANY)
    vmem = pl.BlockSpec(memory_space=pltpu.VMEM)
    scratch = (
        [pltpu.VMEM(flat, BF)] * 3
        + [pltpu.VMEM((chunks, side * rows, order), BF)]
        + [pltpu.VMEM(cube, BF)] * 2
        + [
            pltpu.VMEM((side, rows, order), F32),
            pltpu.VMEM((side, rows, order), F32),
            pltpu.VMEM((blocks, width, cols), BF),
            pltpu.VMEM((peers, share, width), BF),
            pltpu.VMEM((own, out), BF),
            pltpu.VMEM((steps, 2, chips, share, cols), BF),
            pltpu.VMEM((steps, chips, share, cols), BF),
            pltpu.VMEM((steps, across - 1, chips // across, share, cols), BF),
            pltpu.VMEM((steps, chips // across - 1, share, cols), BF),
            pltpu.VMEM((steps, peers, share, cols), BF),
            pltpu.VMEM((parts, tokens // parts, width), F32),
            pltpu.VMEM((order, order), F32),
            pltpu.VMEM((side, side), F32),
            pltpu.VMEM(piece, F32),
            pltpu.VMEM(piece, BF),
            pltpu.VMEM(piece, BF),
            pltpu.VMEM((layers, deep, lanes), F32),
            pltpu.VMEM((deep, lanes), BF),
        ]
        + [dma, dma((chunks,))] * 2
        + [dma((chunks,))] * 2
        + [dma] * 2
        + [dma((blocks,)), dma]
        + [dma, dma((steps,))] * 6
        + [dma] * 6
    )
    grad, sums = pl.pallas_call(
        kernel,
        out_shape=[jax.ShapeDtypeStruct(flat, BF), jax.ShapeDtypeStruct(piece, BF)],
        in_specs=[hbm, vmem, vmem, vmem, hbm, hbm],
        out_specs=[hbm, hbm],
        scratch_shapes=scratch,
        compiler_params=pltpu.CompilerParams(
            collective_id=0, has_side_effects=True, vmem_limit_bytes=67043328
        ),
    )(
        activations.reshape(flat), left_factor, right_factor, clip_scale.T,
        weight_rows, target.reshape(peers, own, out),
    )
    input_grad, left_sum, right_sum = finish(
        grad.reshape(tokens, width), sums.reshape(peers * deep, lanes), order, side
    )
    return (left_sum, right_sum, input_grad)


def solution(mesh):
    placed = (P("dp", "tensor"), P(), P(), P(), P("tensor", None), P("dp", None))
    return jax.shard_map(
        local, mesh=mesh, in_specs=placed, out_specs=(P(), P(), P("dp", "tensor")), check_vma=False
    )
```

```python
import jax
import jax.numpy as jnp
from jax import lax
from jax.experimental import pallas as pl
from jax.experimental.pallas import tpu as pltpu
from jax.sharding import PartitionSpec as P

BF = jnp.bfloat16
F32 = jnp.float32
MESH = pl.DeviceIdType.MESH
LAGS = (0, 1, 3, 5, 7, 9, 10)


def split(value):
    head = value.astype(BF)
    return head, (value - head.astype(F32)).astype(BF)


def dot(a, b, dims):
    return lax.dot_general(a, b, ((dims[:1], dims[1:]), ((), ())), preferred_element_type=F32)


def remote(src, dst, send, recv, **where):
    return pltpu.make_async_remote_copy(
        src_ref=src, dst_ref=dst, send_sem=send, recv_sem=recv,
        device_id=where, device_id_type=MESH,
    )


def wait_for(ref, sem):
    pltpu.make_async_copy(ref, ref, sem).wait()


def others(me, count, body):
    @pl.loop(1, count)
    def _(o):
        body(lax.rem(me + o, count))


def kernel(
    act_ref, left_in, right_in, clip_in, weight_ref, target_ref,
    out_ref, sums_ref,
    left_ref, right_ref, clip_ref,
    x_ref, send_ref, recv_ref,
    tall_ref, mixed_ref, slope_ref, rows_ref, cube_ref,
    w_ref, lhs_ref, aim_ref, part_ref, pair_ref, got_ref, last_ref, grad_ref, acc_ref,
    left_acc, right_acc, stack_ref, terms_ref, shares_ref, layers_ref, total_ref,
    few_sem, in_send, in_recv, fwd_send, fwd_recv, bwd_send, bwd_recv, end_send, end_recv,
    w_sem, aim_sem, pair_send, pair_recv, got_send, got_recv, last_send, last_recv,
    all_send, near_recv, relay_send, far_recv, twins_send, twins_recv,
    share_send, share_recv, layer_send, layer_recv, sum_send, sum_recv,
):
    peers, chunks, rows, width = act_ref.shape
    own = chunks * rows
    order, side = left_ref.shape[0], right_ref.shape[0]
    each = width // order
    blocks, cols = w_ref.shape[0], w_ref.shape[2]
    chips = peers // 2
    layers = layers_ref.shape[0]
    parts, tokens = acc_ref.shape[:2]
    share = tokens // peers
    batch = chunks // parts
    steps = parts * blocks
    wide, high = got_ref.shape[1] + 1, got_ref.shape[2]
    across = wide
    me, layer = lax.axis_index("tensor"), lax.axis_index("dp")
    chip, core = me // 2, lax.rem(me, 2)
    partner = me + 1 - 2 * core
    most = pl.ds(0, peers - 1)

    def unpack(ref, s, c):
        flat = ref[s, c].astype(F32)
        return jnp.concatenate(
            [flat[:, j * order : (j + 1) * order] for j in range(each)], axis=0
        )

    def pack(ref, s, c, value):
        flat = jnp.concatenate(
            [value[j * rows : (j + 1) * rows] for j in range(each)], axis=1
        )
        ref[s, c] = flat.astype(BF)

    def spread(src, dst, send, recv, c):
        pltpu.make_async_copy(src.at[me, c], dst.at[me, c], recv).start()
        others(me, peers, lambda p: remote(
            src.at[p, c], dst.at[me, c], send, recv, tensor=p).start())

    def load_w(n):
        here = pl.ds(pl.multiple_of(n * cols, cols), cols)
        return pltpu.make_async_copy(weight_ref.at[:, here], w_ref.at[n], w_sem.at[n])

    load_aim = pltpu.make_async_copy(target_ref.at[me], aim_ref, aim_sem)

    barrier = pltpu.get_barrier_semaphore()
    others(me, peers, lambda p: pl.semaphore_signal(
        barrier, inc=1, device_id={"tensor": p}, device_id_type=MESH))
    others(layer, layers, lambda d: pl.semaphore_signal(
        barrier, inc=1, device_id={"dp": d}, device_id_type=MESH))
    pl.semaphore_wait(barrier, peers + layers - 2)

    @pl.loop(0, chunks)
    def _(c):
        spread(act_ref, x_ref, in_send, in_recv.at[c], c)

    few = [
        pltpu.make_async_copy(src, dst, few_sem.at[k])
        for k, (src, dst) in enumerate(
            ((left_in, left_ref), (right_in, right_ref), (clip_in, clip_ref))
        )
    ]
    for copy in few:
        copy.start()
    load_aim.start()

    @pl.loop(0, blocks)
    def _(n):
        load_w(n).start()

    for copy in few:
        copy.wait()
    left_hi, left_lo = split(left_ref[...])
    turned_hi, turned_lo = split(jnp.transpose(right_ref[...]))
    turned_wide = jnp.concatenate([turned_hi, turned_hi, turned_lo], axis=1)
    right_hi = right_ref[...].astype(BF)
    clip = jnp.transpose(clip_ref[...])
    unclip = 1.0 / clip

    def forward():
        @pl.loop(0, chunks)
        def _(c):
            wait_for(x_ref.at[:, c], in_recv.at[c])

            @pl.loop(0, peers)
            def _(s):
                x = unpack(x_ref, s, c).astype(BF)
                here = pl.ds(pl.multiple_of(s * each * rows, each * rows), each * rows)
                tall_ref[c, here] = x
                mixed = dot(x, left_hi, (1, 0)) + dot(x, left_lo, (1, 0))
                for j in range(each):
                    rows_ref[s * each + j] = mixed[j * rows : (j + 1) * rows]

            @pl.loop(0, rows, unroll=4)
            def _(t):
                mixed = rows_ref[:, t, :]
                hi, lo = split(mixed)
                mixed_ref[c * rows + t] = hi
                rotated = dot(turned_wide, jnp.concatenate([hi, lo, hi], axis=0), (1, 0))
                bounded = jnp.tanh(rotated * unclip)
                slope_ref[c * rows + t] = (1.0 - bounded * bounded).astype(BF)
                cube_ref[:, t, :] = clip * bounded

            @pl.loop(0, peers)
            def _(s):
                here = pl.ds(pl.multiple_of(s * each, each), each)
                pack(send_ref, s, c, cube_ref[here].reshape(each * rows, order))

            spread(send_ref, recv_ref, fwd_send, fwd_recv.at[c], c)

    def project():
        acc_ref[...] = jnp.zeros_like(acc_ref)
        load_aim.wait()

        halves = 1 if chunks % 2 else 2
        few, deep = chunks // halves, own // halves

        def arrive(half):
            for k in range(few):
                c = half * few + k
                wait_for(recv_ref.at[:, c], fwd_recv.at[c])

            @pl.loop(0, peers)
            def _(s):
                lhs_ref[half, s] = jnp.concatenate(
                    [recv_ref[s, half * few + k] for k in range(few)], axis=0
                )

        def multiply(n, half):
            if half == 0:
                load_w(n).wait()
            lhs = jnp.concatenate([lhs_ref[half, s] for s in range(peers)], axis=0)
            full = dot(lhs, w_ref[n], (1, 0))
            here = slice(half * deep, (half + 1) * deep)
            for p in range(peers):
                part_ref[n, p % 2, p // 2, here] = full[p * deep : (p + 1) * deep].astype(BF)

        for half in range(halves):
            arrive(half)
            if half < halves - 1:
                pl.loop(0, blocks)(lambda n: multiply(n, half))

        def places(n):
            row, col = chip // across, lax.rem(chip, across)
            if across * across != chips:
                return col, row, lambda near, far: far * across + near
            turn = lax.rem(n, 2)

            def at(near, far):
                return (1 - turn) * (far * across + near) + turn * (near * across + far)

            return (1 - turn) * col + turn * row, (1 - turn) * row + turn * col, at

        def stage(i, lag):
            return pl.when((i >= lag) & (i < steps + lag))

        @pl.loop(0, steps + LAGS[6])
        def _(i):
            @stage(i, LAGS[0])
            def _():
                n = i - LAGS[0]
                multiply(n, halves - 1)
                remote(
                    part_ref.at[n, 1 - core], pair_ref.at[n], pair_send, pair_recv.at[n],
                    tensor=partner,
                ).start()

            @stage(i, LAGS[1])
            def _():
                n = i - LAGS[1]
                wait_for(pair_ref.at[n], pair_recv.at[n])
                part_ref[n, core] = (
                    part_ref[n, core].astype(F32) + pair_ref[n].astype(F32)
                ).astype(BF)
                near, far, at = places(n)
                for o in range(1, wide):
                    there = lax.rem(near + o, wide)
                    for k in range(high):
                        remote(
                            part_ref.at[n, core, at(there, k)], got_ref.at[n, o - 1, k],
                            got_send, got_recv.at[n], tensor=2 * at(there, far) + core,
                        ).start()

            @stage(i, LAGS[2])
            def _():
                n = i - LAGS[2]
                near, far, at = places(n)
                wait_for(got_ref.at[n], got_recv.at[n])
                for o in range(1, high):
                    there = lax.rem(far + o, high)
                    block = part_ref.at[n, core, at(near, there)]
                    total = block[...].astype(F32)
                    for k in range(wide - 1):
                        total = total + got_ref[n, k, there].astype(F32)
                    block[...] = total.astype(BF)
                    remote(
                        block, last_ref.at[n, o - 1], last_send, last_recv.at[n],
                        tensor=2 * at(near, there) + core,
                    ).start()

            @stage(i, LAGS[3])
            def _():
                n = i - LAGS[3]
                near, far, at = places(n)
                wait_for(last_ref.at[n], last_recv.at[n])
                total = part_ref[n, core, chip].astype(F32)
                for k in range(wide - 1):
                    total = total + got_ref[n, k, far].astype(F32)
                for k in range(high - 1):
                    total = total + last_ref[n, k].astype(F32)
                part, block = n // blocks, lax.rem(n, blocks)
                here = pl.ds(pl.multiple_of(block * cols, cols), cols)
                aim = aim_ref[pl.ds(pl.multiple_of(part * share, share), share), here]
                grad_ref[n, me] = (total - aim.astype(F32)).astype(BF)
                mine = grad_ref.at[n, me]
                for o in range(1, wide):
                    remote(
                        mine, mine, all_send, near_recv.at[n],
                        tensor=2 * at(lax.rem(near + o, wide), far) + core,
                    ).start()
                for o in range(1, high):
                    remote(
                        mine, mine, all_send, far_recv.at[n],
                        tensor=2 * at(near, lax.rem(far + o, high)) + core,
                    ).start()
                remote(mine, mine, all_send, twins_recv.at[n], tensor=partner).start()

            @stage(i, LAGS[4])
            def _():
                n = i - LAGS[4]
                near, far, at = places(n)
                wait_for(grad_ref.at[n, pl.ds(0, wide - 1)], near_recv.at[n])
                for o in range(1, wide):
                    block = grad_ref.at[n, 2 * at(lax.rem(near + o, wide), far) + core]
                    for k in range(1, high):
                        remote(
                            block, block, relay_send, far_recv.at[n],
                            tensor=2 * at(near, lax.rem(far + k, high)) + core,
                        ).start()
                    remote(block, block, twins_send, twins_recv.at[n], tensor=partner).start()

            @stage(i, LAGS[5])
            def _():
                n = i - LAGS[5]
                near, far, at = places(n)
                wait_for(grad_ref.at[n, pl.ds(0, (high - 1) * wide)], far_recv.at[n])
                for o in range(1, high):
                    for k in range(wide):
                        block = grad_ref.at[n, 2 * at(k, lax.rem(far + o, high)) + core]
                        remote(block, block, twins_send, twins_recv.at[n], tensor=partner).start()

            @stage(i, LAGS[6])
            def _():
                n = i - LAGS[6]
                wait_for(grad_ref.at[n, pl.ds(0, chips)], twins_recv.at[n])
                part, block = n // blocks, lax.rem(n, blocks)
                grad = jnp.concatenate([grad_ref[n, s] for s in range(peers)], axis=0)
                for h in range(0, width, 512):
                    here = slice(h, min(h + 512, width))
                    acc_ref[part, :, here] += dot(grad, w_ref[block, here, :], (1, 1))

                @pl.when(n == blocks - 1)
                def _():
                    wait_for(send_ref.at[most], fwd_send)

                @pl.when(block == blocks - 1)
                def _():
                    for k in range(batch):
                        c = part * batch + k

                        @pl.loop(0, peers)
                        def _(p):
                            start = pl.multiple_of(p * share + k * rows, rows)
                            send_ref[p, c] = acc_ref[part, pl.ds(start, rows), :].astype(BF)

                        spread(send_ref, recv_ref, bwd_send.at[c], bwd_recv.at[c], c)

    def drain_forward():
        wait_for(x_ref.at[most], in_send)

    def backward():
        left_acc[...] = jnp.zeros_like(left_acc)
        right_acc[...] = jnp.zeros_like(right_acc)
        stack_ref[...] = jnp.zeros_like(stack_ref)

        @pl.loop(0, chunks)
        def _(c):
            wait_for(recv_ref.at[:, c], bwd_recv.at[c])

            @pl.loop(0, peers)
            def _(s):
                here = pl.ds(pl.multiple_of(s * each, each), each)
                rows_ref[here] = unpack(recv_ref, s, c).reshape(each, rows, order)

            @pl.loop(0, rows, unroll=4)
            def _(t):
                turned = (rows_ref[:, t, :] * slope_ref[c * rows + t].astype(F32)).astype(BF)
                right_acc[...] += dot(mixed_ref[c * rows + t], turned, (1, 1))
                cube_ref[:, t, :] = dot(right_hi, turned, (1, 0))

            unmixed = cube_ref[...].reshape(side * rows, order).astype(BF)
            left_acc[...] += dot(tall_ref[c], unmixed, (0, 0))

            @pl.when(c == chunks - 1)
            def _():
                deep = stack_ref.shape[1]
                half = side // 2
                for g in range(order // 8):
                    p, at = divmod(g * 8, deep)
                    stack_ref[p, at : at + 8, :order] = left_acc[g * 8 : (g + 1) * 8]
                for g in range(half // 8):
                    p, at = divmod(order + g * 8, deep)
                    top = right_acc[g * 8 : (g + 1) * 8]
                    low = right_acc[half + g * 8 : half + (g + 1) * 8]
                    stack_ref[p, at : at + 8, :side] = top
                    stack_ref[p, at : at + 8, side : 2 * side] = low
                terms_ref[...] = stack_ref[...].astype(BF)
                for o in range(1, peers):
                    p = lax.rem(me + o, peers)
                    remote(
                        terms_ref.at[p], shares_ref.at[o - 1], share_send, share_recv, tensor=p
                    ).start()

                @pl.loop(1, chunks - 1)
                def _(k):
                    spread(send_ref, out_ref, end_send, end_recv, k)

            wait_for(send_ref.at[most, c], bwd_send.at[c])

            @pl.loop(0, peers)
            def _(s):
                here = pl.ds(pl.multiple_of(s * each, each), each)
                unmixed = cube_ref[here].reshape(each * rows, order).astype(BF)
                pack(send_ref, s, c, dot(unmixed, left_hi, (1, 1)))

            if chunks > 1:

                @pl.when(c == 0)
                def _():
                    spread(send_ref, out_ref, end_send, end_recv, c)

    def combine():
        wait_for(shares_ref.at[most], share_recv)
        total = stack_ref[me]
        for o in range(1, peers):
            total = total + shares_ref[o - 1].astype(F32)
        layers_ref[layer] = total
        mine = layers_ref.at[layer]
        others(layer, layers, lambda d: remote(
            mine, mine, layer_send, layer_recv, dp=d).start())
        wait_for(layers_ref.at[pl.ds(0, layers - 1)], layer_recv)
        total = layers_ref[0]
        for d in range(1, layers):
            total = total + layers_ref[d]
        total_ref[...] = total.astype(BF)
        pltpu.make_async_copy(total_ref, sums_ref.at[me], sum_recv).start()
        others(me, peers, lambda p: remote(
            total_ref, sums_ref.at[me], sum_send, sum_recv, tensor=p).start())
        spread(send_ref, out_ref, end_send, end_recv, chunks - 1)

        wait_for(sums_ref, sum_recv)
        wait_for(layers_ref.at[pl.ds(0, layers - 1)], layer_send)
        wait_for(shares_ref.at[most], share_send)
        wait_for(shares_ref.at[most], sum_send)

    def drain_ends():
        wait_for(out_ref, end_recv)
        wait_for(send_ref.at[most], end_send)

    def drain_blocks():
        wait_for(part_ref.at[:, 0], pair_send)
        wait_for(got_ref, got_send)
        wait_for(last_ref, last_send)
        wait_for(grad_ref.at[:, pl.ds(0, wide + high - 1)], all_send)
        wait_for(grad_ref.at[:, pl.ds(0, (wide - 1) * (high - 1))], relay_send)
        wait_for(grad_ref.at[:, pl.ds(0, chips - 1)], twins_send)

    forward()
    project()
    drain_forward()
    backward()
    combine()
    drain_ends()
    drain_blocks()


def finish_kernel(
    grad_ref, sums_ref, out_ref, left_ref, right_ref,
    in_buf, out_buf, sums_buf, left_buf, right_buf, in_sem, out_sem, few_sem,
):
    steps = in_buf.shape[0]

    def load(i):
        return pltpu.make_async_copy(grad_ref.at[i], in_buf.at[i], in_sem.at[i])

    def store(i):
        return pltpu.make_async_copy(out_buf.at[i], out_ref.at[i], out_sem.at[i])

    for i in range(steps):
        load(i).start()
    load_sums = pltpu.make_async_copy(sums_ref, sums_buf, few_sem.at[0])
    load_sums.start()
    for i in range(steps):
        load(i).wait()
        out_buf[i] = in_buf[i].astype(F32)
        store(i).start()
    order, side = left_buf.shape[0], right_buf.shape[0]
    half = side // 2
    load_sums.wait()
    left_buf[...] = sums_buf[:order, :order].astype(F32)
    right_buf[:half] = sums_buf[order : order + half, :side].astype(F32)
    right_buf[half:] = sums_buf[order : order + half, side : 2 * side].astype(F32)
    store_left = pltpu.make_async_copy(left_buf, left_ref, few_sem.at[1])
    store_right = pltpu.make_async_copy(right_buf, right_ref, few_sem.at[2])
    store_left.start()
    store_right.start()
    for i in range(steps):
        store(i).wait()
    store_left.wait()
    store_right.wait()


def finish(grad, sums, order, side):
    tokens, width = grad.shape
    steps = tokens // 32
    split_up = (steps, 32, width)
    hbm = pl.BlockSpec(memory_space=pl.ANY)
    out, left, right = pl.pallas_call(
        finish_kernel,
        in_specs=[hbm, hbm],
        out_specs=[hbm, hbm, hbm],
        out_shape=[
            jax.ShapeDtypeStruct(split_up, F32),
            jax.ShapeDtypeStruct((order, order), F32),
            jax.ShapeDtypeStruct((side, side), F32),
        ],
        scratch_shapes=[
            pltpu.VMEM(split_up, BF),
            pltpu.VMEM(split_up, F32),
            pltpu.VMEM(sums.shape, BF),
            pltpu.VMEM((order, order), F32),
            pltpu.VMEM((side, side), F32),
            pltpu.SemaphoreType.DMA((steps,)),
            pltpu.SemaphoreType.DMA((steps,)),
            pltpu.SemaphoreType.DMA((3,)),
        ],
    )(grad.reshape(split_up), sums)
    return out.reshape(tokens, width), left, right


def local(activations, left_factor, right_factor, clip_scale, weight_rows, target):
    peers, layers = lax.axis_size("tensor"), lax.axis_size("dp")
    tokens, width = activations.shape
    order, side = left_factor.shape[0], right_factor.shape[0]
    out = weight_rows.shape[1]
    own = tokens // peers
    rows = min(own, 8)
    chunks = own // rows
    chips = peers // 2
    across = max(b for b in range(1, chips + 1) if chips % b == 0 and b * b <= chips)
    across = chips // across
    cols = next(b for b in (512, 256, 128) if out % b == 0)
    blocks = out // cols
    parts, halves = 1, 1 if chunks % 2 else 2
    steps, share = parts * blocks, own // parts
    lanes = -(-max(order, 2 * side) // 128) * 128
    deep = -(-(order + side // 2) // (8 * peers)) * 8
    flat = (peers, chunks, rows, width)
    cube = (own, side, order)
    piece = (peers, deep, lanes)
    dma = pltpu.SemaphoreType.DMA
    hbm = pl.BlockSpec(memory_space=pl.ANY)
    scratch = (
        [pltpu.VMEM((order, order), F32), pltpu.VMEM((side, side), F32), pltpu.VMEM((order, side), F32)]
        + [pltpu.VMEM(flat, BF)] * 3
        + [pltpu.VMEM((chunks, side * rows, order), BF)]
        + [pltpu.VMEM(cube, BF)] * 2
        + [
            pltpu.VMEM((side, rows, order), F32),
            pltpu.VMEM((side, rows, order), F32),
            pltpu.VMEM((blocks, width, cols), BF),
            pltpu.VMEM((halves, peers, own // halves, width), BF),
            pltpu.VMEM((own, out), BF),
            pltpu.VMEM((steps, 2, chips, share, cols), BF),
            pltpu.VMEM((steps, chips, share, cols), BF),
            pltpu.VMEM((steps, across - 1, chips // across, share, cols), BF),
            pltpu.VMEM((steps, chips // across - 1, share, cols), BF),
            pltpu.VMEM((steps, peers, share, cols), BF),
            pltpu.VMEM((parts, tokens // parts, width), F32),
            pltpu.VMEM((order, order), F32),
            pltpu.VMEM((side, side), F32),
            pltpu.VMEM(piece, F32),
            pltpu.VMEM(piece, BF),
            pltpu.VMEM(piece, BF),
            pltpu.VMEM((layers, deep, lanes), F32),
            pltpu.VMEM((deep, lanes), BF),
        ]
        + [dma((3,))]
        + [dma, dma((chunks,))] * 2
        + [dma((chunks,))] * 2
        + [dma] * 2
        + [dma((blocks,)), dma]
        + [dma, dma((steps,))] * 6
        + [dma] * 6
    )
    grad, sums = pl.pallas_call(
        kernel,
        out_shape=[jax.ShapeDtypeStruct(flat, BF), jax.ShapeDtypeStruct(piece, BF)],
        in_specs=[hbm] * 6,
        out_specs=[hbm, hbm],
        scratch_shapes=scratch,
        compiler_params=pltpu.CompilerParams(
            collective_id=0, has_side_effects=True, vmem_limit_bytes=67043328
        ),
    )(
        activations.reshape(flat), left_factor, right_factor, clip_scale.T,
        weight_rows, target.reshape(peers, own, out),
    )
    input_grad, left_sum, right_sum = finish(
        grad.reshape(tokens, width), sums.reshape(peers * deep, lanes), order, side
    )
    return (left_sum, right_sum, input_grad)


def solution(mesh):
    placed = (P("dp", "tensor"), P(), P(), P(), P("tensor", None), P("dp", None))
    return jax.shard_map(
        local, mesh=mesh, in_specs=placed, out_specs=(P(), P(), P("dp", "tensor")), check_vma=False
    )
```

```python
import jax
import jax.numpy as jnp
from jax import lax
from jax.experimental import pallas as pl
from jax.experimental.pallas import tpu as pltpu
from jax.sharding import PartitionSpec as P

BF = jnp.bfloat16
F32 = jnp.float32
MESH = pl.DeviceIdType.MESH
LAGS = (0, 1, 3, 5, 7, 9, 10)


def split(value):
    head = value.astype(BF)
    return head, (value - head.astype(F32)).astype(BF)


def dot(a, b, dims):
    return lax.dot_general(a, b, ((dims[:1], dims[1:]), ((), ())), preferred_element_type=F32)


def remote(src, dst, send, recv, **where):
    return pltpu.make_async_remote_copy(
        src_ref=src, dst_ref=dst, send_sem=send, recv_sem=recv,
        device_id=where, device_id_type=MESH,
    )


def wait_for(ref, sem):
    pltpu.make_async_copy(ref, ref, sem).wait()


def others(me, count, body):
    @pl.loop(1, count)
    def _(o):
        body(lax.rem(me + o, count))


def kernel(
    act_ref, left_in, right_in, clip_in, weight_ref, target_ref,
    out_ref, sums_ref,
    left_ref, right_ref, clip_ref,
    x_ref, send_ref, recv_ref,
    tall_ref, mixed_ref, slope_ref, rows_ref, cube_ref,
    w_ref, lhs_ref, aim_ref, part_ref, pair_ref, got_ref, last_ref, grad_ref, acc_ref,
    left_acc, right_acc, stack_ref, terms_ref, shares_ref, layers_ref, total_ref,
    few_sem, in_send, in_recv, fwd_send, fwd_recv, bwd_send, bwd_recv, end_send, end_recv,
    w_sem, aim_sem, pair_send, pair_recv, got_send, got_recv, last_send, last_recv,
    all_send, near_recv, relay_send, far_recv, twins_send, twins_recv,
    share_send, share_recv, layer_send, layer_recv, sum_send, sum_recv,
):
    peers, chunks, rows, width = act_ref.shape
    own = chunks * rows
    order, side = left_ref.shape[0], right_ref.shape[0]
    each = width // order
    blocks, cols = w_ref.shape[0], w_ref.shape[2]
    chips = peers // 2
    layers = layers_ref.shape[0]
    parts, tokens = acc_ref.shape[:2]
    share = tokens // peers
    batch = chunks // parts
    steps = parts * blocks
    wide, high = got_ref.shape[1] + 1, got_ref.shape[2]
    across = wide
    me, layer = lax.axis_index("tensor"), lax.axis_index("dp")
    chip, core = me // 2, lax.rem(me, 2)
    partner = me + 1 - 2 * core
    most = pl.ds(0, peers - 1)

    def unpack(ref, s, c):
        flat = ref[s, c].astype(F32)
        return jnp.concatenate(
            [flat[:, j * order : (j + 1) * order] for j in range(each)], axis=0
        )

    def pack(ref, s, c, value):
        flat = jnp.concatenate(
            [value[j * rows : (j + 1) * rows] for j in range(each)], axis=1
        )
        ref[s, c] = flat.astype(BF)

    def spread(src, dst, send, recv, c):
        pltpu.make_async_copy(src.at[me, c], dst.at[me, c], recv).start()
        others(me, peers, lambda p: remote(
            src.at[p, c], dst.at[me, c], send, recv, tensor=p).start())

    def load_w(n):
        here = pl.ds(pl.multiple_of(n * cols, cols), cols)
        return pltpu.make_async_copy(weight_ref.at[:, here], w_ref.at[n], w_sem.at[n])

    load_aim = pltpu.make_async_copy(target_ref.at[me], aim_ref, aim_sem)

    barrier = pltpu.get_barrier_semaphore()
    others(me, peers, lambda p: pl.semaphore_signal(
        barrier, inc=1, device_id={"tensor": p}, device_id_type=MESH))
    others(layer, layers, lambda d: pl.semaphore_signal(
        barrier, inc=1, device_id={"dp": d}, device_id_type=MESH))
    pl.semaphore_wait(barrier, peers + layers - 2)

    @pl.loop(0, chunks)
    def _(c):
        spread(act_ref, x_ref, in_send, in_recv.at[c], c)

    few = [
        pltpu.make_async_copy(src, dst, few_sem.at[k])
        for k, (src, dst) in enumerate(
            ((left_in, left_ref), (right_in, right_ref), (clip_in, clip_ref))
        )
    ]
    for copy in few:
        copy.start()
    load_aim.start()

    @pl.loop(0, blocks)
    def _(n):
        load_w(n).start()

    for copy in few:
        copy.wait()
    left_hi, left_lo = split(left_ref[...])
    turned_hi, turned_lo = split(jnp.transpose(right_ref[...]))
    turned_wide = jnp.concatenate([turned_hi, turned_hi, turned_lo], axis=1)
    right_hi = right_ref[...].astype(BF)
    clip = jnp.transpose(clip_ref[...])
    unclip = 1.0 / clip

    def forward():
        @pl.loop(0, chunks)
        def _(c):
            wait_for(x_ref.at[:, c], in_recv.at[c])

            @pl.loop(0, peers)
            def _(s):
                x = unpack(x_ref, s, c).astype(BF)
                here = pl.ds(pl.multiple_of(s * each * rows, each * rows), each * rows)
                tall_ref[c, here] = x
                mixed = dot(x, left_hi, (1, 0)) + dot(x, left_lo, (1, 0))
                for j in range(each):
                    rows_ref[s * each + j] = mixed[j * rows : (j + 1) * rows]

            @pl.loop(0, rows, unroll=8)
            def _(t):
                mixed = rows_ref[:, t, :]
                hi, lo = split(mixed)
                mixed_ref[c * rows + t] = hi
                rotated = dot(turned_wide, jnp.concatenate([hi, lo, hi], axis=0), (1, 0))
                bounded = jnp.tanh(rotated * unclip)
                slope_ref[c * rows + t] = (1.0 - bounded * bounded).astype(BF)
                cube_ref[:, t, :] = clip * bounded

            @pl.loop(0, peers)
            def _(s):
                here = pl.ds(pl.multiple_of(s * each, each), each)
                pack(send_ref, s, c, cube_ref[here].reshape(each * rows, order))

            spread(send_ref, recv_ref, fwd_send, fwd_recv.at[c], c)

    def project():
        acc_ref[...] = jnp.zeros_like(acc_ref)
        load_aim.wait()

        halves = 1 if chunks % 2 else 2
        few, deep = chunks // halves, own // halves

        def arrive(half):
            for k in range(few):
                c = half * few + k
                wait_for(recv_ref.at[:, c], fwd_recv.at[c])

            @pl.loop(0, peers)
            def _(s):
                lhs_ref[half, s] = jnp.concatenate(
                    [recv_ref[s, half * few + k] for k in range(few)], axis=0
                )

        def multiply(n, half):
            if half == 0:
                load_w(n).wait()
            lhs = jnp.concatenate([lhs_ref[half, s] for s in range(peers)], axis=0)
            full = dot(lhs, w_ref[n], (1, 0))
            here = slice(half * deep, (half + 1) * deep)
            for p in range(peers):
                part_ref[n, p % 2, p // 2, here] = full[p * deep : (p + 1) * deep].astype(BF)

        for half in range(halves):
            arrive(half)
            if half < halves - 1:
                pl.loop(0, blocks)(lambda n: multiply(n, half))

        def places(n):
            row, col = chip // across, lax.rem(chip, across)
            if across * across != chips:
                return col, row, lambda near, far: far * across + near
            turn = lax.rem(n, 2)

            def at(near, far):
                return (1 - turn) * (far * across + near) + turn * (near * across + far)

            return (1 - turn) * col + turn * row, (1 - turn) * row + turn * col, at

        def stage(i, lag):
            return pl.when((i >= lag) & (i < steps + lag))

        @pl.loop(0, steps + LAGS[6])
        def _(i):
            @stage(i, LAGS[0])
            def _():
                n = i - LAGS[0]
                multiply(n, halves - 1)
                remote(
                    part_ref.at[n, 1 - core], pair_ref.at[n], pair_send, pair_recv.at[n],
                    tensor=partner,
                ).start()

            @stage(i, LAGS[1])
            def _():
                n = i - LAGS[1]
                wait_for(pair_ref.at[n], pair_recv.at[n])
                part_ref[n, core] = (
                    part_ref[n, core].astype(F32) + pair_ref[n].astype(F32)
                ).astype(BF)
                near, far, at = places(n)
                for o in range(1, wide):
                    there = lax.rem(near + o, wide)
                    for k in range(high):
                        remote(
                            part_ref.at[n, core, at(there, k)], got_ref.at[n, o - 1, k],
                            got_send, got_recv.at[n], tensor=2 * at(there, far) + core,
                        ).start()

            @stage(i, LAGS[2])
            def _():
                n = i - LAGS[2]
                near, far, at = places(n)
                wait_for(got_ref.at[n], got_recv.at[n])
                for o in range(1, high):
                    there = lax.rem(far + o, high)
                    block = part_ref.at[n, core, at(near, there)]
                    total = block[...].astype(F32)
                    for k in range(wide - 1):
                        total = total + got_ref[n, k, there].astype(F32)
                    block[...] = total.astype(BF)
                    remote(
                        block, last_ref.at[n, o - 1], last_send, last_recv.at[n],
                        tensor=2 * at(near, there) + core,
                    ).start()

            @stage(i, LAGS[3])
            def _():
                n = i - LAGS[3]
                near, far, at = places(n)
                wait_for(last_ref.at[n], last_recv.at[n])
                total = part_ref[n, core, chip].astype(F32)
                for k in range(wide - 1):
                    total = total + got_ref[n, k, far].astype(F32)
                for k in range(high - 1):
                    total = total + last_ref[n, k].astype(F32)
                part, block = n // blocks, lax.rem(n, blocks)
                here = pl.ds(pl.multiple_of(block * cols, cols), cols)
                aim = aim_ref[pl.ds(pl.multiple_of(part * share, share), share), here]
                grad_ref[n, me] = (total - aim.astype(F32)).astype(BF)
                mine = grad_ref.at[n, me]
                for o in range(1, wide):
                    remote(
                        mine, mine, all_send, near_recv.at[n],
                        tensor=2 * at(lax.rem(near + o, wide), far) + core,
                    ).start()
                for o in range(1, high):
                    remote(
                        mine, mine, all_send, far_recv.at[n],
                        tensor=2 * at(near, lax.rem(far + o, high)) + core,
                    ).start()
                remote(mine, mine, all_send, twins_recv.at[n], tensor=partner).start()

            @stage(i, LAGS[4])
            def _():
                n = i - LAGS[4]
                near, far, at = places(n)
                wait_for(grad_ref.at[n, pl.ds(0, wide - 1)], near_recv.at[n])
                for o in range(1, wide):
                    block = grad_ref.at[n, 2 * at(lax.rem(near + o, wide), far) + core]
                    for k in range(1, high):
                        remote(
                            block, block, relay_send, far_recv.at[n],
                            tensor=2 * at(near, lax.rem(far + k, high)) + core,
                        ).start()
                    remote(block, block, twins_send, twins_recv.at[n], tensor=partner).start()

            @stage(i, LAGS[5])
            def _():
                n = i - LAGS[5]
                near, far, at = places(n)
                wait_for(grad_ref.at[n, pl.ds(0, (high - 1) * wide)], far_recv.at[n])
                for o in range(1, high):
                    for k in range(wide):
                        block = grad_ref.at[n, 2 * at(k, lax.rem(far + o, high)) + core]
                        remote(block, block, twins_send, twins_recv.at[n], tensor=partner).start()

            @stage(i, LAGS[6])
            def _():
                n = i - LAGS[6]
                wait_for(grad_ref.at[n, pl.ds(0, chips)], twins_recv.at[n])
                part, block = n // blocks, lax.rem(n, blocks)
                grad = jnp.concatenate([grad_ref[n, s] for s in range(peers)], axis=0)
                for h in range(0, width, 512):
                    here = slice(h, min(h + 512, width))
                    acc_ref[part, :, here] += dot(grad, w_ref[block, here, :], (1, 1))

                @pl.when(n == blocks - 1)
                def _():
                    wait_for(send_ref.at[most], fwd_send)

                @pl.when(block == blocks - 1)
                def _():
                    for k in range(batch):
                        c = part * batch + k

                        @pl.loop(0, peers)
                        def _(p):
                            start = pl.multiple_of(p * share + k * rows, rows)
                            send_ref[p, c] = acc_ref[part, pl.ds(start, rows), :].astype(BF)

                        spread(send_ref, recv_ref, bwd_send.at[c], bwd_recv.at[c], c)

    def drain_forward():
        wait_for(x_ref.at[most], in_send)

    def backward():
        left_acc[...] = jnp.zeros_like(left_acc)
        right_acc[...] = jnp.zeros_like(right_acc)
        stack_ref[...] = jnp.zeros_like(stack_ref)

        @pl.loop(0, chunks)
        def _(c):
            wait_for(recv_ref.at[:, c], bwd_recv.at[c])

            @pl.loop(0, peers)
            def _(s):
                here = pl.ds(pl.multiple_of(s * each, each), each)
                rows_ref[here] = unpack(recv_ref, s, c).reshape(each, rows, order)

            @pl.loop(0, rows, unroll=8)
            def _(t):
                turned = (rows_ref[:, t, :] * slope_ref[c * rows + t].astype(F32)).astype(BF)
                right_acc[...] += dot(mixed_ref[c * rows + t], turned, (1, 1))
                cube_ref[:, t, :] = dot(right_hi, turned, (1, 0))

            unmixed = cube_ref[...].reshape(side * rows, order).astype(BF)
            left_acc[...] += dot(tall_ref[c], unmixed, (0, 0))

            @pl.when(c == chunks - 1)
            def _():
                deep = stack_ref.shape[1]
                half = side // 2
                for g in range(order // 8):
                    p, at = divmod(g * 8, deep)
                    stack_ref[p, at : at + 8, :order] = left_acc[g * 8 : (g + 1) * 8]
                for g in range(half // 8):
                    p, at = divmod(order + g * 8, deep)
                    top = right_acc[g * 8 : (g + 1) * 8]
                    low = right_acc[half + g * 8 : half + (g + 1) * 8]
                    stack_ref[p, at : at + 8, :side] = top
                    stack_ref[p, at : at + 8, side : 2 * side] = low
                terms_ref[...] = stack_ref[...].astype(BF)
                for o in range(1, peers):
                    p = lax.rem(me + o, peers)
                    remote(
                        terms_ref.at[p], shares_ref.at[o - 1], share_send, share_recv, tensor=p
                    ).start()

                @pl.loop(1, chunks - 1)
                def _(k):
                    spread(send_ref, out_ref, end_send, end_recv, k)

            wait_for(send_ref.at[most, c], bwd_send.at[c])

            @pl.loop(0, peers)
            def _(s):
                here = pl.ds(pl.multiple_of(s * each, each), each)
                unmixed = cube_ref[here].reshape(each * rows, order).astype(BF)
                pack(send_ref, s, c, dot(unmixed, left_hi, (1, 1)))

            if chunks > 1:

                @pl.when(c == 0)
                def _():
                    spread(send_ref, out_ref, end_send, end_recv, c)

    def combine():
        wait_for(shares_ref.at[most], share_recv)
        total = stack_ref[me]
        for o in range(1, peers):
            total = total + shares_ref[o - 1].astype(F32)
        layers_ref[layer] = total
        mine = layers_ref.at[layer]
        others(layer, layers, lambda d: remote(
            mine, mine, layer_send, layer_recv, dp=d).start())
        wait_for(layers_ref.at[pl.ds(0, layers - 1)], layer_recv)
        total = layers_ref[0]
        for d in range(1, layers):
            total = total + layers_ref[d]
        total_ref[...] = total.astype(BF)
        pltpu.make_async_copy(total_ref, sums_ref.at[me], sum_recv).start()
        others(me, peers, lambda p: remote(
            total_ref, sums_ref.at[me], sum_send, sum_recv, tensor=p).start())
        spread(send_ref, out_ref, end_send, end_recv, chunks - 1)

        wait_for(sums_ref, sum_recv)
        wait_for(layers_ref.at[pl.ds(0, layers - 1)], layer_send)
        wait_for(shares_ref.at[most], share_send)
        wait_for(shares_ref.at[most], sum_send)

    def drain_ends():
        wait_for(out_ref, end_recv)
        wait_for(send_ref.at[most], end_send)

    def drain_blocks():
        wait_for(part_ref.at[:, 0], pair_send)
        wait_for(got_ref, got_send)
        wait_for(last_ref, last_send)
        wait_for(grad_ref.at[:, pl.ds(0, wide + high - 1)], all_send)
        wait_for(grad_ref.at[:, pl.ds(0, (wide - 1) * (high - 1))], relay_send)
        wait_for(grad_ref.at[:, pl.ds(0, chips - 1)], twins_send)

    forward()
    project()
    drain_forward()
    backward()
    combine()
    drain_ends()
    drain_blocks()


def finish_kernel(
    grad_ref, sums_ref, out_ref, left_ref, right_ref,
    in_buf, out_buf, sums_buf, left_buf, right_buf, in_sem, out_sem, few_sem,
):
    steps = in_buf.shape[0]

    def load(i):
        return pltpu.make_async_copy(grad_ref.at[i], in_buf.at[i], in_sem.at[i])

    def store(i):
        return pltpu.make_async_copy(out_buf.at[i], out_ref.at[i], out_sem.at[i])

    for i in range(steps):
        load(i).start()
    load_sums = pltpu.make_async_copy(sums_ref, sums_buf, few_sem.at[0])
    load_sums.start()
    for i in range(steps):
        load(i).wait()
        out_buf[i] = in_buf[i].astype(F32)
        store(i).start()
    order, side = left_buf.shape[0], right_buf.shape[0]
    half = side // 2
    load_sums.wait()
    left_buf[...] = sums_buf[:order, :order].astype(F32)
    right_buf[:half] = sums_buf[order : order + half, :side].astype(F32)
    right_buf[half:] = sums_buf[order : order + half, side : 2 * side].astype(F32)
    store_left = pltpu.make_async_copy(left_buf, left_ref, few_sem.at[1])
    store_right = pltpu.make_async_copy(right_buf, right_ref, few_sem.at[2])
    store_left.start()
    store_right.start()
    for i in range(steps):
        store(i).wait()
    store_left.wait()
    store_right.wait()


def finish(grad, sums, order, side):
    tokens, width = grad.shape
    steps = tokens // 32
    split_up = (steps, 32, width)
    hbm = pl.BlockSpec(memory_space=pl.ANY)
    out, left, right = pl.pallas_call(
        finish_kernel,
        in_specs=[hbm, hbm],
        out_specs=[hbm, hbm, hbm],
        out_shape=[
            jax.ShapeDtypeStruct(split_up, F32),
            jax.ShapeDtypeStruct((order, order), F32),
            jax.ShapeDtypeStruct((side, side), F32),
        ],
        scratch_shapes=[
            pltpu.VMEM(split_up, BF),
            pltpu.VMEM(split_up, F32),
            pltpu.VMEM(sums.shape, BF),
            pltpu.VMEM((order, order), F32),
            pltpu.VMEM((side, side), F32),
            pltpu.SemaphoreType.DMA((steps,)),
            pltpu.SemaphoreType.DMA((steps,)),
            pltpu.SemaphoreType.DMA((3,)),
        ],
    )(grad.reshape(split_up), sums)
    return out.reshape(tokens, width), left, right


def local(activations, left_factor, right_factor, clip_scale, weight_rows, target):
    peers, layers = lax.axis_size("tensor"), lax.axis_size("dp")
    tokens, width = activations.shape
    order, side = left_factor.shape[0], right_factor.shape[0]
    out = weight_rows.shape[1]
    own = tokens // peers
    rows = min(own, 8)
    chunks = own // rows
    chips = peers // 2
    across = max(b for b in range(1, chips + 1) if chips % b == 0 and b * b <= chips)
    across = chips // across
    cols = next(b for b in (512, 256, 128) if out % b == 0)
    blocks = out // cols
    parts, halves = 1, 1 if chunks % 2 else 2
    steps, share = parts * blocks, own // parts
    lanes = -(-max(order, 2 * side) // 128) * 128
    deep = -(-(order + side // 2) // (8 * peers)) * 8
    flat = (peers, chunks, rows, width)
    cube = (own, side, order)
    piece = (peers, deep, lanes)
    dma = pltpu.SemaphoreType.DMA
    hbm = pl.BlockSpec(memory_space=pl.ANY)
    scratch = (
        [pltpu.VMEM((order, order), F32), pltpu.VMEM((side, side), F32), pltpu.VMEM((order, side), F32)]
        + [pltpu.VMEM(flat, BF)] * 3
        + [pltpu.VMEM((chunks, side * rows, order), BF)]
        + [pltpu.VMEM(cube, BF)] * 2
        + [
            pltpu.VMEM((side, rows, order), F32),
            pltpu.VMEM((side, rows, order), F32),
            pltpu.VMEM((blocks, width, cols), BF),
            pltpu.VMEM((halves, peers, own // halves, width), BF),
            pltpu.VMEM((own, out), BF),
            pltpu.VMEM((steps, 2, chips, share, cols), BF),
            pltpu.VMEM((steps, chips, share, cols), BF),
            pltpu.VMEM((steps, across - 1, chips // across, share, cols), BF),
            pltpu.VMEM((steps, chips // across - 1, share, cols), BF),
            pltpu.VMEM((steps, peers, share, cols), BF),
            pltpu.VMEM((parts, tokens // parts, width), F32),
            pltpu.VMEM((order, order), F32),
            pltpu.VMEM((side, side), F32),
            pltpu.VMEM(piece, F32),
            pltpu.VMEM(piece, BF),
            pltpu.VMEM(piece, BF),
            pltpu.VMEM((layers, deep, lanes), F32),
            pltpu.VMEM((deep, lanes), BF),
        ]
        + [dma((3,))]
        + [dma, dma((chunks,))] * 2
        + [dma((chunks,))] * 2
        + [dma] * 2
        + [dma((blocks,)), dma]
        + [dma, dma((steps,))] * 6
        + [dma] * 6
    )
    grad, sums = pl.pallas_call(
        kernel,
        out_shape=[jax.ShapeDtypeStruct(flat, BF), jax.ShapeDtypeStruct(piece, BF)],
        in_specs=[hbm] * 6,
        out_specs=[hbm, hbm],
        scratch_shapes=scratch,
        compiler_params=pltpu.CompilerParams(
            collective_id=0, has_side_effects=True, vmem_limit_bytes=67043328
        ),
    )(
        activations.reshape(flat), left_factor, right_factor, clip_scale.T,
        weight_rows, target.reshape(peers, own, out),
    )
    input_grad, left_sum, right_sum = finish(
        grad.reshape(tokens, width), sums.reshape(peers * deep, lanes), order, side
    )
    return (left_sum, right_sum, input_grad)


def solution(mesh):
    placed = (P("dp", "tensor"), P(), P(), P(), P("tensor", None), P("dp", None))
    return jax.shard_map(
        local, mesh=mesh, in_specs=placed, out_specs=(P(), P(), P("dp", "tensor")), check_vma=False
    )
```
